32 devices in a mesh: win: 8 (over z, y), tile: 4 (over x, core).
Axes of the slice: x: 2, y: 2, z: 4, core: 2. Of those that a mesh axis runs over, the one named last changes fastest.
Arguments:
- right_side: float32 [8, 2, 128, 1024], P('win', None, 'tile'), may hold values from -64 to 64
- error_weight: float32 [8, 2, 128, 1024], P('win', None, 'tile'), may hold values from 0.5 to 4
- coeffs: float32 [4, 8, 2, 128, 1024], P(None, 'win', None, 'tile'), may hold values from 0.1 to 0.4
- obs_block: int32 [8, 128], P('win', 'tile'), may hold values from 0 to 511
- obs_pos: int32 [8, 128, 128], P('win', 'tile'), may hold values from 0 to 127
- obs_weight: float32 [8, 128, 128], P('win', 'tile'), may hold values from 0.5 to 4
Outputs:
- solution_field: float32 [8, 2, 128, 1024], P('win', None, 'tile')
- residual: float32 [8, 2, 128, 1024], P('win', None, 'tile')
The draws below stay inside these ranges and needn't reach their ends.
All inputs are finite; a program needn't handle non-finite values.
Results may differ from the reference program's by a relative error of at most 0.0001.
Values sent between devices are 32-bit elements; how exact they have to be, the bound alone decides.
A program may use at most 64 MiB of HBM per device.

```python
import math
import jax
import jax.numpy as jnp

LEV = 2
TY = 32
NX = 1024
NBLK = 32
OBSW = 128
ITERS = 3
NWIN = 8
NY = 128
BROWS = 512
N_TILE = 4


def draw_right_side(key, part):
    gaussian = jax.random.normal(jax.random.fold_in(key, 11), (NWIN, LEV, NY, NX), jnp.float32)
    gaussian = jnp.clip(gaussian, -6.0, 6.0)
    growth = 1.0 + 2.0 * jnp.arange(NWIN, dtype=jnp.float32) / max(NWIN - 1, 1)
    growth = growth.reshape(NWIN, 1, 1, 1)
    return growth * gaussian


def place_ends(entries, own_key, low, top_value):
    longest = entries.shape.index(max(entries.shape))
    spots = []
    for shift in (0, 1):
        where = [jax.random.randint(jax.random.fold_in(own_key, axis), (), 0, length) for axis, length in enumerate(entries.shape)]
        where[longest] = (where[longest] + shift) % entries.shape[longest]
        spots.append(tuple(where))
    return entries.at[spots[0]].set(low).at[spots[1]].set(top_value)


def block_levels(key, extent, pieces, smallest, largest):
    def one(axis_at, shards_of):
        heights = jax.random.uniform(jax.random.fold_in(jax.random.fold_in(key, 6), axis_at), (shards_of,), jnp.float32, smallest / len(pieces), largest / len(pieces))
        return jnp.repeat(jnp.exp(heights), extent[axis_at] // shards_of).reshape((-1,) + (1,) * (len(extent) - axis_at - 1))

    level = one(*pieces[0])
    for cut in pieces[1:]:
        level = level * one(*cut)
    return level


def setup_inputs(seed: int = 0) -> dict:
    seeds = jax.random.split(jax.random.key(seed), 7)
    right_side = draw_right_side(jax.random.fold_in(seeds[6], 71), 0)
    error_weight = jnp.clip(jnp.exp(math.log(4.0) - 2.0794415 * jax.random.uniform(seeds[1], (NWIN, LEV, NY, NX), jnp.float32) ** block_levels(seeds[1], (NWIN, LEV, NY, NX), ((0, 8), (2, 4)), -0.2, 0.2)), 0.5, 4.0)
    coeffs = jnp.clip(0.1 + 0.3 * jax.random.uniform(seeds[2], (4, NWIN, LEV, NY, NX), jnp.float32) ** block_levels(seeds[2], (4, NWIN, LEV, NY, NX), ((1, 8), (3, 4)), -0.2, 0.2), 0.1, 0.4)
    obs_block = place_ends(jax.random.randint(seeds[3], (NWIN, N_TILE * NBLK), 0, BROWS), jax.random.fold_in(seeds[3], 1), 0, BROWS - 1).astype(jnp.int32)
    obs_pos = place_ends(jax.random.randint(seeds[4], (NWIN, N_TILE * NBLK, OBSW), 0, OBSW), jax.random.fold_in(seeds[4], 1), 0, OBSW - 1).astype(jnp.int32)
    obs_weight = jnp.clip(jnp.exp(math.log(4.0) - 2.0794415 * jax.random.uniform(seeds[5], (NWIN, N_TILE * NBLK, OBSW), jnp.float32) ** block_levels(seeds[5], (NWIN, N_TILE * NBLK, OBSW), ((0, 8), (1, 4)), -0.2, 0.2)), 0.5, 4.0)
    return {"right_side": right_side, "error_weight": error_weight, "coeffs": coeffs, "obs_block": obs_block, "obs_pos": obs_pos, "obs_weight": obs_weight}


def model_step(state, coeffs):
    padded = jnp.pad(state, ((0, 0), (0, 0), (1, 1), (0, 0)))
    north_south = padded[:, :, 2:, :] + padded[:, :, :-2, :]
    return (coeffs[0] * state + coeffs[1] * north_south
            + coeffs[2] * jnp.roll(state, -1, axis=3) + coeffs[3] * jnp.roll(state, 1, axis=3))


def model_adjoint(state, coeffs):
    spread = jnp.pad(coeffs[1] * state, ((0, 0), (0, 0), (1, 1), (0, 0)))
    north_south = spread[:, :, 2:, :] + spread[:, :, :-2, :]
    return (coeffs[0] * state + north_south
            + jnp.roll(coeffs[2] * state, 1, axis=3) + jnp.roll(coeffs[3] * state, -1, axis=3))


def observe(state, obs_block, obs_pos, obs_weight):
    windows = state.shape[0]
    cell_count = LEV * TY * NX
    blocks = state.reshape(windows, LEV, N_TILE, TY, NX).transpose(0, 2, 1, 3, 4).reshape(windows, N_TILE, cell_count)
    flat_index = (obs_block.reshape(windows, N_TILE, NBLK, 1).astype(jnp.int32) * OBSW
                  + obs_pos.reshape(windows, N_TILE, NBLK, OBSW).astype(jnp.int32))
    flat_index = flat_index.reshape(windows, N_TILE, NBLK * OBSW).astype(jnp.int32)
    observed = jnp.take_along_axis(blocks, flat_index, axis=2)
    weighted = observed * obs_weight.reshape(windows, N_TILE, NBLK * OBSW)

    def place(index_row, value_row):
        return jnp.zeros((cell_count,), jnp.float32).at[index_row].add(value_row)

    spread = jax.vmap(jax.vmap(place))(flat_index, weighted)
    return spread.reshape(windows, N_TILE, LEV, TY, NX).transpose(0, 2, 1, 3, 4).reshape(windows, LEV, NY, NX)


def reference(right_side, error_weight, coeffs, obs_block, obs_pos, obs_weight):
    def hessian(state):
        propagated = model_step(state, coeffs)
        before = jnp.concatenate([jnp.zeros_like(propagated[:1]), propagated[:-1]], axis=0)
        weighted = error_weight * (state - before)
        following = jnp.concatenate([weighted[1:], jnp.zeros_like(weighted[:1])], axis=0)
        return weighted - model_adjoint(following, coeffs) + observe(state, obs_block, obs_pos, obs_weight)

    solution_field = jnp.zeros_like(right_side)
    residual = right_side
    direction = right_side
    norm_now = jnp.sum(residual * residual)
    for iteration in range(ITERS):
        product_vec = hessian(direction)
        step_length = norm_now / jnp.sum(direction * product_vec)
        solution_field = solution_field + step_length * direction
        residual = residual - step_length * product_vec
        norm_next = jnp.sum(residual * residual)
        direction = residual + (norm_next / norm_now) * direction
        norm_now = norm_next
    return solution_field, residual
```

```python
import functools

import jax
import jax.numpy as jnp
from jax import lax
from jax.experimental import pallas as pl
from jax.experimental.pallas import tpu as pltpu
from jax.sharding import PartitionSpec as P

ITERS = 3
EDGE = 8


def doubling(length):
    steps, known = [], 1
    while known < length - 1:
        steps.append(known)
        known *= 2
    return steps


def kernel(wins, tiles, rhs, err, cof, oblk_in, opos_in, owgt_in, x_out, r_out,
           obk, ops, owt, v, y, w, wn, c, d, ob, u, ui, vn, z, eo, ei, go, gi, rt, home, tail, part, red,
           x_sem, xs_sem, l_sem, h_send, h_recv, b_send, b_recv, g_send, g_recv,
           rt_send, rt_recv, rd_send, rd_recv, wn_send, wn_recv, hello):
    me_w = lax.axis_index("win")
    me_t = lax.axis_index("tile")
    lev = lax.rem(me_w, 2)
    other = 1 - lev
    mate = me_w + 1 - 2 * lev
    has_next = me_w + 2 < wins
    has_prev = me_w >= 2
    has_north = me_t > 0
    has_south = me_t < tiles - 1
    rows, cols = v.shape[2], v.shape[3]
    oblk, opos, owgt = obk, ops, owt
    count = wins * tiles
    me = me_w * tiles + me_t
    width = opos.shape[2]
    nblk = opos.shape[1]

    def remote(src, dst, ssem, rsem, win, tile):
        return pltpu.make_async_remote_copy(
            src_ref=src, dst_ref=dst, send_sem=ssem, recv_sem=rsem,
            device_id=(win, tile), device_id_type=pl.DeviceIdType.MESH)

    pieces = [(0, EDGE), (rows - EDGE, EDGE)] + [
        (lo, EDGE) for lo in range(EDGE, rows - EDGE, EDGE)]
    many = len(pieces)

    barrier = pltpu.get_barrier_semaphore()

    def signal(sem, win, tile):
        pl.semaphore_signal(sem, inc=1, device_id=(win, tile), device_id_type=pl.DeviceIdType.MESH)

    def greet(sem, ends):
        for there, win, tile in ends:
            pl.when(there)(functools.partial(signal, sem, win, tile))

    def met(sem, ends):
        pl.semaphore_wait(sem, sum(there.astype(jnp.int32) for there, _, _ in ends))

    def along_tile(step):
        return [(me_t >= step, me_w, me_t - step), (me_t + step < tiles, me_w, me_t + step)]

    def along_win(step):
        return [(me_w >= 2 * step, me_w - 2 * step, me_t),
                (me_w + 2 * step < wins, me_w + 2 * step, me_t)]

    facing = [(me_w >= 0, mate, me_t)]
    near = facing + along_tile(1) + along_win(1)
    rounds = ([along_tile(step) for step in doubling(tiles)] + [facing]
              + [along_win(step) for step in doubling(wins // 2)])
    turn = iter(range(len(rounds) + 1))

    def spread():
        at = next(turn, None)
        if at is None:
            return
        if at > 0:
            met(hello.at[at - 1], rounds[at - 1])
        if at < len(rounds):
            greet(hello.at[at], rounds[at])

    greet(barrier, near)

    swaps = [
        remote(rhs.at[0, other], v.at[0, lev], xs_sem.at[0], x_sem.at[0], mate, me_t),
        remote(err.at[0, other], w.at[lev], xs_sem.at[1], x_sem.at[1], mate, me_t),
    ] + [
        remote(cof.at[:, 0, other, pl.ds(lo, n)], c.at[:, lev, pl.ds(lo, n)],
               xs_sem.at[3 + k], x_sem.at[3 + k], mate, me_t)
        for k, (lo, n) in enumerate(pieces)
    ]
    locs = [
        pltpu.make_async_copy(oblk_in, obk, l_sem.at[4]),
        pltpu.make_async_copy(opos_in, ops, l_sem.at[5]),
        pltpu.make_async_copy(owgt_in, owt, l_sem.at[6]),
        pltpu.make_async_copy(rhs.at[0, lev], v.at[0, lev], l_sem.at[0]),
        pltpu.make_async_copy(err.at[0, lev], w.at[lev], l_sem.at[1]),
        pltpu.make_async_copy(rhs.at[0, other], home, l_sem.at[2]),
        pltpu.make_async_copy(cof.at[:, 0, lev], c.at[:, lev], l_sem.at[3]),
    ]
    for s in locs:
        s.start()
    locs = locs[3:] + locs[:3]
    met(barrier, near)
    for s in swaps[:3]:
        s.start()
    spread()

    @pl.when(jnp.logical_not(has_north))
    def _():
        for it in range(ITERS):
            ei[it, 0] = jnp.zeros(ei.shape[2:], jnp.float32)
            gi[it, 0] = jnp.zeros(gi.shape[2:], jnp.float32)

    @pl.when(jnp.logical_not(has_south))
    def _():
        for it in range(ITERS):
            ei[it, 1] = jnp.zeros(ei.shape[2:], jnp.float32)
            gi[it, 1] = jnp.zeros(gi.shape[2:], jnp.float32)

    @pl.when(jnp.logical_not(has_prev))
    def _():
        for it in range(ITERS):
            ui[it] = jnp.zeros(ui.shape[1:], jnp.float32)

    @pl.when(jnp.logical_not(has_next))
    def _():
        wn[...] = jnp.zeros(wn.shape, jnp.float32)
        for it in range(ITERS):
            vn[it] = jnp.zeros(vn.shape[1:], jnp.float32)

    for s in locs[4:]:
        s.wait()
    cell = lax.broadcasted_iota(jnp.int32, (width, width), 0)
    ones = jnp.ones((8, width), jnp.float32)
    ob[lev, nblk:, :] = jnp.zeros((8, width), jnp.float32)

    def per_block(b, carry):
        hit = jnp.where(cell == opos[0, pl.ds(b, 1), :], owgt[0, pl.ds(b, 1), :], 0.0)
        total = lax.dot_general(ones, hit, (((1,), (1,)), ((), ())),
                                precision=lax.Precision.HIGHEST,
                                preferred_element_type=jnp.float32)
        ob[lev, pl.ds(b, 1), :] = total[0:1]
        return carry

    lax.fori_loop(0, nblk, per_block, 0)
    ob[lev, nblk:nblk + 1, 0:nblk] = oblk[...].astype(jnp.float32)
    ob_copy = remote(ob.at[lev], ob.at[lev], xs_sem.at[2], x_sem.at[2], mate, me_t)
    ob_copy.start()
    spread()

    states = (v.at[0], y.at[0], v.at[1])

    def arrived(k):
        return [
            lambda: remote(rhs.at[0, other], v.at[0, other], xs_sem.at[0], x_sem.at[0], mate, me_t),
            lambda: remote(err.at[0, other], w.at[other], xs_sem.at[1], x_sem.at[1], mate, me_t),
        ][k]()


    def edge_copies(out, into, ssem, rsem, it):
        north = remote(out.at[it, 0], into.at[it, 1], ssem.at[it, 0], rsem.at[it, 1],
                       me_w, me_t - 1)
        south = remote(out.at[it, 1], into.at[it, 0], ssem.at[it, 1], rsem.at[it, 0],
                       me_w, me_t + 1)
        return north, south

    def edges_start(out, into, ssem, rsem, it):
        north, south = edge_copies(out, into, ssem, rsem, it)
        pl.when(has_north)(north.start)
        pl.when(has_south)(south.start)

    def edges_wait_recv(out, into, ssem, rsem, it):
        north, south = edge_copies(out, into, ssem, rsem, it)
        pl.when(has_north)(south.wait_recv)
        pl.when(has_south)(north.wait_recv)

    def edges_wait_send(out, into, ssem, rsem, it):
        north, south = edge_copies(out, into, ssem, rsem, it)
        pl.when(has_north)(north.wait_send)
        pl.when(has_south)(south.wait_send)

    def back_copy(it, k):
        lo, n = pieces[k]
        return remote(states[it].at[0, pl.ds(lo, n)], vn.at[it, pl.ds(lo, n)],
                      b_send.at[0, it, k], b_recv.at[0, it, k], me_w - 2, me_t)

    def forth_copy(it, k):
        lo, n = pieces[k]
        return remote(u.at[1, pl.ds(lo, n)], ui.at[it, pl.ds(lo, n)],
                      b_send.at[1, it, k], b_recv.at[1, it, k], me_w + 2, me_t)

    def ret_copy(it):
        return remote(y.at[it, other], rt.at[it], rt_send.at[it], rt_recv.at[it], mate, me_t)

    row = lax.broadcasted_iota(jnp.int32, (rows, cols), 0)
    row8 = lax.broadcasted_iota(jnp.int32, (EDGE, cols), 0)

    def above(a):
        return jnp.where(row == 0, 0.0, pltpu.roll(a, 1, 0))

    def below(a):
        return jnp.where(row == rows - 1, 0.0, pltpu.roll(a, rows - 1, 0))

    def east(a):
        return pltpu.roll(a, cols - 1, 1)

    def west(a):
        return pltpu.roll(a, 1, 1)

    last = rows - 1
    wn_copy = remote(w.at[0], wn, wn_send, wn_recv, me_w - 2, me_t)

    def model_piece(it, i, k):
        lo, n = pieces[k]
        src = states[it]
        a = src[i, lo:lo + n]
        top = ei[it, 0, i:i + 1] if lo == 0 else src[i, lo - 1:lo]
        bottom = ei[it, 1, i:i + 1] if lo + n == rows else src[i, lo + n:lo + n + 1]
        sides = (jnp.where(row8 == 0, top, pltpu.roll(a, 1, 0))
                 + jnp.where(row8 == n - 1, bottom, pltpu.roll(a, n - 1, 0)))
        u[i, lo:lo + n] = (c[0, i, lo:lo + n] * a + c[1, i, lo:lo + n] * sides
                           + c[2, i, lo:lo + n] * east(a) + c[3, i, lo:lo + n] * west(a))

    def sends(it):
        src = states[it]
        for i in range(2):
            eo[it, 0, i:i + 1] = src[i, 0:1]
            eo[it, 1, i:i + 1] = src[i, last:last + 1]
        edges_start(eo, ei, h_send, h_recv, it)

        @pl.when(has_prev)
        def _():
            for k in range(many):
                back_copy(it, k).start()

    def product(it, beside):
        src = states[it]
        sends(it)
        if it > 0:
            beside()
        if it == 0:
            locs[1].wait()
            arrived(1).wait_recv()
            for later in swaps[3:4]:
                later.start()
            pl.when(has_prev)(wn_copy.start)
            locs[3].wait()
            edges_wait_recv(eo, ei, h_send, h_recv, it)
            for k in range(many):
                spread()
                swaps[2 + k].wait_recv()
                for later in swaps[4 + k:5 + k]:
                    later.start()
                model_piece(it, 1, k)
                pl.when(has_next)(forth_copy(it, k).start)
                model_piece(it, 0, k)
                if k == 1:
                    adjoint_edges(it)
                    beside()
        else:
            @pl.when(has_next)
            def _():
                for k in range(many):
                    forth_copy(it - 1, k).wait_send()

            for k in range(2, many):
                model_piece(it, 1, k)
                pl.when(has_next)(forth_copy(it, k).start)
            edges_wait_recv(eo, ei, h_send, h_recv, it)
            for k in range(2):
                model_piece(it, 1, k)
                pl.when(has_next)(forth_copy(it, k).start)
            for k in range(2):
                model_piece(it, 0, k)
            adjoint_edges(it)
            for k in range(2, many):
                model_piece(it, 0, k)

        def adjoint(i, q):
            g = c[1, i] * q
            return (c[0, i] * q + (above(g) + below(g)) + west(c[2, i] * q) + east(c[3, i] * q))

        z[...] = w[1] * (src[1] - u[0])
        y[it, 0] = d[0] * src[0] - adjoint(0, z[...])

        @pl.when(has_next)
        def _():
            for k in range(2, many):
                back_copy(it, k).wait_recv()

        y[it, 1] = (z[...] + d[1] * src[1]) - adjoint(1, wn[...] * (vn[it] - u[1]))

        edges_wait_recv(go, gi, g_send, g_recv, it)
        for i in range(2):
            y[it, i, 0:1] = y[it, i, 0:1] - gi[it, 0, i:i + 1]
            y[it, i, last:last + 1] = y[it, i, last:last + 1] - gi[it, 1, i:i + 1]

        @pl.when(has_prev)
        def _():
            for k in range(many):
                forth_copy(it, k).wait_recv()

        y[it, 0] = y[it, 0] + w[0] * (src[0] - ui[it])

    def adjoint_edges(it):
        src = states[it]

        @pl.when(has_next)
        def _():
            if it == 0:
                wn_copy.wait_recv()
            back_copy(it, 0).wait_recv()
            back_copy(it, 1).wait_recv()

        for side, at in ((0, 0), (1, last)):
            here = slice(at, at + 1)
            go[it, side, 0:1] = c[1, 0, here] * (w[1, here] * (src[1, here] - u[0, here]))
            go[it, side, 1:2] = c[1, 1, here] * (wn[here] * (vn[it, here] - u[1, here]))
        edges_start(go, gi, g_send, g_recv, it)

    def lanes(pair):
        a = jnp.sum(pair[0] + pair[1], axis=0, keepdims=True)
        total = a[:, 0:128]
        for k in range(1, cols // 128):
            total = total + a[:, k * 128:(k + 1) * 128]
        return total

    def reduce_start(it, r, aw):
        part[it, 0:1] = lanes(r * r)
        part[it, 1:2] = lanes(r * aw)

        def send(o, carry):
            to = lax.rem(me + o, count)
            remote(part.at[it], red.at[it, me], rd_send.at[it], rd_recv.at[it],
                   to // tiles, lax.rem(to, tiles)).start()
            return carry

        lax.fori_loop(1, count, send, 0)
        red[it, me] = part[it]

    def reduce_end(it):
        most = red.at[it, pl.ds(0, count - 1)]
        pltpu.make_async_copy(most, most, rd_recv.at[it]).wait()
        total = jnp.sum(red[it], axis=0)
        both = jnp.sum(total, axis=1, keepdims=True)
        return both[0:1], both[1:2]

    locs[0].wait()
    arrived(0).wait_recv()

    def diagonal():
        remote(ob.at[lev], ob.at[other], xs_sem.at[2], x_sem.at[2], mate, me_t).wait_recv()
        per_row = cols // width
        base = lev * (rows * per_row)
        spot = lax.broadcasted_iota(jnp.int32, (rows, nblk), 0) * per_row + base
        for i in range(2):
            who = ob[i, nblk:nblk + 1, 0:nblk]
            sums = ob[i, 0:nblk, :]
            for k in range(per_row):
                hot = jnp.where((spot + k).astype(jnp.float32) == who, 1.0, 0.0)
                d[i, :, k * width:(k + 1) * width] = jnp.dot(
                    hot, sums, precision=lax.Precision.HIGHEST,
                    preferred_element_type=jnp.float32)

    product(0, diagonal)
    for _ in range(len(rounds)):
        spread()

    def first_sums():
        ret_copy(0).start()
        reduce_start(0, v[0], y[0])

    product(1, first_sums)
    g0, d0 = reduce_end(0)
    a0 = g0 / d0
    v[1] = y[0] - a0 * y[1]

    def second_sums():
        ret_copy(1).start()
        reduce_start(1, v[0] - a0 * y[0], v[1])

    product(2, second_sums)
    g1, d1 = reduce_end(1)
    b1 = g1 / g0
    a1 = g1 / (d1 - b1 * g1 / a0)

    def second(r0, w0, n0, n1):
        r1 = r0 - a0 * w0
        w1 = w0 - a0 * n0
        s1 = w1 + b1 * w0
        r2 = r1 - a1 * s1
        w2 = w1 - a1 * (n1 + b1 * n0)
        return r1, s1, r2, w2

    _, _, r2, w2 = second(v[0], y[0], y[1], y[2])
    reduce_start(2, r2, w2)
    ret_copy(2).start()

    def prepare(level, r0, w0, n0, n1):
        r1, s1, r2, w2 = second(r0, w0, n0, n1)
        p1 = r1 + b1 * r0
        x_out[0, level] = a0 * r0 + a1 * p1
        r_out[0, level] = r2
        tail[2, level] = p1
        tail[0, level] = s1
        tail[1, level] = w2

    def finish(level):
        r2 = r_out[0, level]
        x_out[0, level] = x_out[0, level] + a2 * (r2 + b2 * tail[2, level])
        r_out[0, level] = r2 - a2 * (tail[1, level] + b2 * tail[0, level])

    prepare(lev, v[0, lev], y[0, lev], y[1, lev], y[2, lev])
    locs[2].wait()
    for it in range(ITERS):
        ret_copy(it).wait_recv()
    prepare(other, home[...], rt[0], rt[1], rt[2])
    g2, d2 = reduce_end(2)
    b2 = g2 / g1
    a2 = g2 / (d2 - b2 * g2 / a1)

    finish(lev)
    finish(other)

    for s in swaps:
        s.wait_send()
    ob_copy.wait_send()
    pl.when(has_prev)(wn_copy.wait_send)
    for it in range(ITERS):
        edges_wait_send(eo, ei, h_send, h_recv, it)
        edges_wait_send(go, gi, g_send, g_recv, it)
        ret_copy(it).wait_send()
        most = red.at[it, pl.ds(0, count - 1)]
        pltpu.make_async_copy(most, most, rd_send.at[it]).wait()

        @pl.when(has_prev)
        def _():
            for k in range(many):
                back_copy(it, k).wait_send()

    @pl.when(has_next)
    def _():
        for k in range(many):
            forth_copy(ITERS - 1, k).wait_send()


def on_device(wins, tiles, right_side, error_weight, coeffs, obs_block, obs_pos, obs_weight):
    _, levels, rows, cols = right_side.shape
    nblk, width = obs_pos.shape[1:]
    f32 = jnp.float32
    vm = functools.partial(pltpu.VMEM, dtype=f32)
    dma = pltpu.SemaphoreType.DMA
    anyspace = pl.BlockSpec(memory_space=pltpu.HBM)
    vmem = pl.BlockSpec(memory_space=pltpu.VMEM)
    many = rows // EDGE
    scratch = [
        pltpu.VMEM(obs_block.shape, jnp.int32),
        pltpu.VMEM(obs_pos.shape, jnp.int32),
        vm(obs_weight.shape),
        vm((2, 2, rows, cols)),
        vm((ITERS, 2, rows, cols)),
        vm((2, rows, cols)),
        vm((rows, cols)),
        vm((4, 2, rows, cols)),
        vm((2, rows, cols)),
        vm((2, nblk + 8, width)),
        vm((2, rows, cols)),
        vm((ITERS, rows, cols)),
        vm((ITERS, rows, cols)),
        vm((rows, cols)),
        vm((ITERS, 2, 2, cols)),
        vm((ITERS, 2, 2, cols)),
        vm((ITERS, 2, 2, cols)),
        vm((ITERS, 2, 2, cols)),
        vm((ITERS, rows, cols)),
        vm((rows, cols)),
        vm((3, 2, rows, cols)),
        vm((ITERS, 2, 128)),
        vm((ITERS, wins * tiles, 2, 128)),
        dma((3 + many,)), dma((3 + many,)), dma((7,)),
        dma((ITERS, 2)), dma((ITERS, 2)),
        dma((2, ITERS, many)), dma((2, ITERS, many)),
        dma((ITERS, 2)), dma((ITERS, 2)),
        dma((ITERS,)), dma((ITERS,)),
        dma((ITERS,)), dma((ITERS,)),
        dma, dma,
        pltpu.SemaphoreType.REGULAR((1 + len(doubling(tiles)) + len(doubling(wins // 2)),)),
    ]
    out = vm(right_side.shape)
    return pl.pallas_call(
        functools.partial(kernel, wins, tiles),
        out_shape=(out, out),
        in_specs=[anyspace] * 6,
        out_specs=(vmem, vmem),
        scratch_shapes=scratch,
        compiler_params=pltpu.CompilerParams(has_side_effects=True, collective_id=0,
                                             vmem_limit_bytes=60 * 1024 * 1024),
    )(right_side, error_weight, coeffs, obs_block, obs_pos, obs_weight)


def solution(mesh):
    in_specs = (
        P("win", None, "tile", None),
        P("win", None, "tile", None),
        P(None, "win", None, "tile", None),
        P("win", "tile"),
        P("win", "tile", None),
        P("win", "tile", None),
    )
    out_specs = (P("win", None, "tile", None), P("win", None, "tile", None))
    return jax.shard_map(
        functools.partial(on_device, mesh.shape["win"], mesh.shape["tile"]),
        mesh=mesh, in_specs=in_specs, out_specs=out_specs, check_vma=False
    )
```

```python
import functools

import jax
import jax.numpy as jnp
from jax import lax
from jax.experimental import pallas as pl
from jax.experimental.pallas import tpu as pltpu
from jax.sharding import PartitionSpec as P

ITERS = 3
EDGE = 8
MOMENTS = 2 * ITERS - 1

HOP, BLOCK, SWAP_START, SWAP_FIELD, REDUCE = 2.1, 0.7, 2.0, 2.83, 5.2


def doubling(length):
    steps, known = [], 1
    while known < length - 1:
        steps.append(known)
        known *= 2
    return steps


class Steps:
    def __init__(self):
        self.todo = {}

    def add(self, name, needs, cost, run, sends=None, gets=None):
        self.todo[name] = (list(needs), cost, run, sends, gets)

    def order(self):
        senders = {sends[0]: name for name, (_, _, _, sends, _) in self.todo.items() if sends}
        after = {name: [] for name in self.todo}
        for name, (needs, _, _, _, gets) in self.todo.items():
            for need in needs:
                after[need].append((name, 0.0))
            if gets in senders:
                after[senders[gets]].append((name, self.todo[senders[gets]][3][2]))
        rank = {}

        def path(name):
            if name not in rank:
                rank[name] = self.todo[name][1] + max(
                    (wait + path(then) for then, wait in after[name]), default=0.0)
            return rank[name]

        for name in self.todo:
            path(name)
        now, done, arrive, free, result = 0.0, set(), {}, {}, []
        for _, (_, _, _, _, gets) in self.todo.items():
            if isinstance(gets, tuple) and gets[0] == "at":
                arrive[gets] = gets[1]
        left = dict(self.todo)
        while left:
            ready, soon = None, None
            for name, (needs, _, _, _, gets) in left.items():
                if any(need not in done for need in needs):
                    continue
                at = arrive.get(gets, None) if gets is not None else 0.0
                if at is None:
                    continue
                if at <= now:
                    if ready is None or rank[name] > rank[ready]:
                        ready = name
                elif soon is None or at < soon[0]:
                    soon = (at, name)
            pick = ready
            if pick is None:
                now, pick = soon
            _, cost, run, sends, _ = left.pop(pick)
            now += cost
            done.add(pick)
            if sends:
                message, link, latency, busy = sends
                begin = max(now, free.get(link, 0.0))
                free[link] = begin + busy
                arrive[message] = begin + busy + latency
            result.append((pick, run, now))
        return result


def two_sum(a, b):
    total = a + b
    back = total - a
    return total, (a - (total - back)) + (b - back)


def halves(a):
    big = 4097.0 * a
    high = big - (big - a)
    return high, a - high


def two_product(a, b):
    (ah, al), (bh, bl) = halves(a), halves(b)
    product = a * b
    return product, ((ah * bh - product) + ah * bl + al * bh) + al * bl


def pair_add(a, b):
    total, rest = two_sum(a[0], b[0])
    rest = rest + (a[1] + b[1])
    high = total + rest
    return high, rest - (high - total)


def pair_scale(a, factor):
    product, rest = two_product(a[0], factor)
    rest = rest + a[1] * factor
    high = product + rest
    return high, rest - (high - product)


def pair_rows(a, lo, hi):
    return a[0][lo:hi], a[1][lo:hi]


def pair_total(a):
    return jnp.sum(a[0], axis=1, keepdims=True) + jnp.sum(a[1], axis=1, keepdims=True)


def kernel(wins, tiles, rhs, err, cof, oblk_in, opos_in, owgt_in, x_out, r_out,
           obk, ops, owt, v, y, w, wn, c, d, ob, u, ui, vn, qb, qn, eo, ei, go, gi, rt, home,
           step, grad, early, late, reds, lasts,
           x_sem, xs_sem, l_sem, h_send, h_recv, b_send, b_recv, g_send, g_recv,
           rt_send, rt_recv, rd_send, rd_recv, wn_send, wn_recv, hello):
    me_w = lax.axis_index("win")
    me_t = lax.axis_index("tile")
    lev = lax.rem(me_w, 2)
    other = 1 - lev
    mate = me_w + 1 - 2 * lev
    has_next = me_w + 2 < wins
    has_prev = me_w >= 2
    has_north = me_t > 0
    has_south = me_t < tiles - 1
    rows, cols = v.shape[1], v.shape[2]
    count = wins * tiles
    me = me_w * tiles + me_t
    width = ops.shape[2]
    nblk = ops.shape[1]
    last = rows - 1
    blocks = rows // EDGE
    final = blocks - 1
    pieces = [0, final] + list(range(1, final))
    many = len(pieces)
    f32 = jnp.float32

    def rowset(k):
        return slice(k * EDGE, (k + 1) * EDGE)

    def remote(src, dst, ssem, rsem, win, tile):
        return pltpu.make_async_remote_copy(
            src_ref=src, dst_ref=dst, send_sem=ssem, recv_sem=rsem,
            device_id=(win, tile), device_id_type=pl.DeviceIdType.MESH)

    barrier = pltpu.get_barrier_semaphore()

    def signal(sem, win, tile):
        pl.semaphore_signal(sem, inc=1, device_id=(win, tile), device_id_type=pl.DeviceIdType.MESH)

    def greet(sem, ends):
        for there, win, tile in ends:
            pl.when(there)(functools.partial(signal, sem, win, tile))

    def met(sem, ends):
        pl.semaphore_wait(sem, sum(there.astype(jnp.int32) for there, _, _ in ends))

    def along_tile(hop):
        return [(me_t >= hop, me_w, me_t - hop), (me_t + hop < tiles, me_w, me_t + hop)]

    def along_win(hop):
        return [(me_w >= 2 * hop, me_w - 2 * hop, me_t),
                (me_w + 2 * hop < wins, me_w + 2 * hop, me_t)]

    facing = [(me_w >= 0, mate, me_t)]
    near = facing + along_tile(1) + along_win(1)
    rounds = ([along_tile(hop) for hop in doubling(tiles)] + [facing]
              + [along_win(hop) for hop in doubling(wins // 2)])

    greet(barrier, near)

    swaps = [
        remote(rhs.at[0, other], v.at[lev], xs_sem.at[0], x_sem.at[0], mate, me_t),
        remote(err.at[0, other], w.at[lev], xs_sem.at[1], x_sem.at[1], mate, me_t),
    ] + [
        remote(cof.at[:, 0, other, pl.ds(k * EDGE, EDGE)], c.at[:, lev, pl.ds(k * EDGE, EDGE)],
               xs_sem.at[3 + n], x_sem.at[3 + n], mate, me_t)
        for n, k in enumerate(pieces)
    ]
    arrivals = [
        remote(rhs.at[0, other], v.at[other], xs_sem.at[0], x_sem.at[0], mate, me_t),
        remote(err.at[0, other], w.at[other], xs_sem.at[1], x_sem.at[1], mate, me_t),
    ] + [
        remote(cof.at[:, 0, other, pl.ds(k * EDGE, EDGE)], c.at[:, other, pl.ds(k * EDGE, EDGE)],
               xs_sem.at[3 + n], x_sem.at[3 + n], mate, me_t)
        for n, k in enumerate(pieces)
    ]
    locs = {
        "block": pltpu.make_async_copy(oblk_in, obk, l_sem.at[4]),
        "pos": pltpu.make_async_copy(opos_in, ops, l_sem.at[5]),
        "weight": pltpu.make_async_copy(owgt_in, owt, l_sem.at[6]),
        "rhs": pltpu.make_async_copy(rhs.at[0, lev], v.at[lev], l_sem.at[0]),
        "err": pltpu.make_async_copy(err.at[0, lev], w.at[lev], l_sem.at[1]),
        "home": pltpu.make_async_copy(rhs.at[0, other], home, l_sem.at[2]),
        "cof": pltpu.make_async_copy(cof.at[:, 0, lev], c.at[:, lev], l_sem.at[3]),
    }
    for one in locs.values():
        one.start()
    met(barrier, near)
    for one in swaps[:3]:
        one.start()
    greet(hello.at[0], rounds[0])

    @pl.when(jnp.logical_not(has_north))
    def _():
        for it in range(ITERS):
            ei[it, 0] = jnp.zeros(ei.shape[2:], f32)
            gi[it, 0] = jnp.zeros(gi.shape[2:], f32)

    @pl.when(jnp.logical_not(has_south))
    def _():
        for it in range(ITERS):
            ei[it, 1] = jnp.zeros(ei.shape[2:], f32)
            gi[it, 1] = jnp.zeros(gi.shape[2:], f32)

    @pl.when(jnp.logical_not(has_prev))
    def _():
        for it in range(ITERS):
            ui[it] = jnp.zeros(ui.shape[1:], f32)

    @pl.when(jnp.logical_not(has_next))
    def _():
        wn[...] = jnp.zeros(wn.shape, f32)
        for it in range(ITERS):
            vn[it] = jnp.zeros(vn.shape[1:], f32)

    for one in ("block", "pos", "weight"):
        locs[one].wait()
    cell = lax.broadcasted_iota(jnp.int32, (width, width), 0)
    ones = jnp.ones((8, width), f32)
    ob[lev, nblk:, :] = jnp.zeros((8, width), f32)

    def per_block(b, carry):
        hit = jnp.where(cell == ops[0, pl.ds(b, 1), :], owt[0, pl.ds(b, 1), :], 0.0)
        total = lax.dot_general(ones, hit, (((1,), (1,)), ((), ())),
                                precision=lax.Precision.HIGHEST,
                                preferred_element_type=f32)
        ob[lev, pl.ds(b, 1), :] = total[0:1]
        return carry

    lax.fori_loop(0, nblk, per_block, 0)
    ob[lev, nblk:nblk + 1, 0:nblk] = obk[...].astype(f32)
    ob_copy = remote(ob.at[lev], ob.at[lev], xs_sem.at[2], x_sem.at[2], mate, me_t)
    ob_back = remote(ob.at[lev], ob.at[other], xs_sem.at[2], x_sem.at[2], mate, me_t)
    ob_copy.start()

    states = (v, y.at[0], y.at[1])
    row8 = lax.broadcasted_iota(jnp.int32, (EDGE, cols), 0)
    ways = (has_north, has_south)

    def east(a):
        return pltpu.roll(a, cols - 1, 1)

    def west(a):
        return pltpu.roll(a, 1, 1)

    def sides(a, top, bottom):
        return (jnp.where(row8 == 0, top, pltpu.roll(a, 1, 0))
                + jnp.where(row8 == EDGE - 1, bottom, pltpu.roll(a, EDGE - 1, 0)))

    def edge_copy(out, into, ssem, rsem, it, side):
        return remote(out.at[it, side], into.at[it, 1 - side], ssem.at[it, side],
                      rsem.at[it, 1 - side], me_w, me_t - 1 + 2 * side)

    def edge_in(out, into, ssem, rsem, it, side):
        return remote(out.at[it, 1 - side], into.at[it, side], ssem.at[it, 1 - side],
                      rsem.at[it, side], me_w, me_t - 1 + 2 * side)

    def back_copy(it, k):
        return remote(states[it].at[0, pl.ds(k * EDGE, EDGE)], vn.at[it, pl.ds(k * EDGE, EDGE)],
                      b_send.at[0, it, k], b_recv.at[0, it, k], me_w - 2, me_t)

    def forth_copy(it, k):
        return remote(u.at[it, 1, pl.ds(k * EDGE, EDGE)], ui.at[it, pl.ds(k * EDGE, EDGE)],
                      b_send.at[1, it, k], b_recv.at[1, it, k], me_w + 2, me_t)

    def ret_copy(it, k):
        return remote(y.at[it, other, pl.ds(k * EDGE, EDGE)], rt.at[it, pl.ds(k * EDGE, EDGE)],
                      rt_send.at[it, k], rt_recv.at[it, k], mate, me_t)

    wn_copy = remote(w.at[0], wn, wn_send, wn_recv, me_w - 2, me_t)

    def model(it, i, k):
        src = states[it]
        lo, hi = k * EDGE, (k + 1) * EDGE
        a = src[i, lo:hi]
        top = ei[it, 0, i:i + 1] if k == 0 else src[i, lo - 1:lo]
        bottom = ei[it, 1, i:i + 1] if k == final else src[i, hi:hi + 1]
        u[it, i, lo:hi] = (c[0, i, lo:hi] * a + c[1, i, lo:hi] * sides(a, top, bottom)
                           + c[2, i, lo:hi] * east(a) + c[3, i, lo:hi] * west(a))
        if i == 1:
            pl.when(has_next)(forth_copy(it, k).start)

    def misfit_here(it, k):
        at = rowset(k)
        qb[it, at] = w[1, at] * (states[it][1, at] - u[it, 0, at])

    def misfit_next(it, k):
        at = rowset(k)
        qn[it, at] = wn[at] * (vn[it, at] - u[it, 1, at])

    def adjoint(it, i, q, k, alone=None):
        lo, hi = k * EDGE, (k + 1) * EDGE
        a = q[it, lo:hi]
        if k == 0:
            top = gi[it, 0, i:i + 1]
        elif alone is not None:
            top = jnp.zeros((1, cols), f32)
        else:
            top = c[1, i, lo - 1:lo] * q[it, lo - 1:lo]
        if k == final:
            bottom = gi[it, 1, i:i + 1]
        elif alone is not None:
            bottom = jnp.zeros((1, cols), f32)
        else:
            bottom = c[1, i, hi:hi + 1] * q[it, hi:hi + 1]
        return (c[0, i, lo:hi] * a + sides(c[1, i, lo:hi] * a, top, bottom)
                + west(c[2, i, lo:hi] * a) + east(c[3, i, lo:hi] * a))

    def image(it, i, k, alone=None):
        at = rowset(k)
        src = states[it]
        if i == 1:
            return (qb[it, at] + d[1, at] * src[1, at]) - adjoint(it, 1, qn, k, alone)
        return (d[0, at] * src[0, at] - adjoint(it, 0, qb, k, alone)) + w[0, at] * (src[0, at] - ui[it, at])

    def diagonal():
        ob_back.wait_recv()
        per_row = cols // width
        base = lev * (rows * per_row)
        spot = lax.broadcasted_iota(jnp.int32, (rows, nblk), 0) * per_row + base
        for i in range(2):
            who = ob[i, nblk:nblk + 1, 0:nblk]
            sums = ob[i, 0:nblk, :]
            for k in range(per_row):
                hot = jnp.where((spot + k).astype(f32) == who, 1.0, 0.0)
                d[i, :, k * width:(k + 1) * width] = jnp.dot(
                    hot, sums, precision=lax.Precision.HIGHEST, preferred_element_type=f32)

    def lanes(a, b):
        total = None
        for k in range(blocks):
            at = rowset(k)
            here = a[0, at] * b[0, at] + a[1, at] * b[1, at]
            total = here if total is None else total + here
        total = jnp.sum(total, axis=0, keepdims=True)
        parts = [total[:, k * width:(k + 1) * width] for k in range(cols // width)]
        while len(parts) > 1:
            parts = [sum(parts[k:k + 2]) for k in range(0, len(parts), 2)]
        return parts[0]

    def to_all(part, into, sems):
        def send(o, carry):
            to = lax.rem(me + o, count)
            remote(part, into.at[me], rd_send.at[sems], rd_recv.at[sems],
                   to // tiles, lax.rem(to, tiles)).start()
            return carry

        lax.fori_loop(1, count, send, 0)
        into[me] = part[...]

    def from_all(into, sems):
        most = into.at[pl.ds(0, count - 1)]
        pltpu.make_async_copy(most, most, rd_recv.at[sems]).wait()
        high, low = into[0], jnp.zeros(into.shape[1:], f32)
        for k in range(1, count):
            high, rest = two_sum(high, into[k])
            low = low + rest
        return high, low

    S = Steps()
    scalars = {}

    def spread(at):
        met(hello.at[at], rounds[at])
        if at + 1 < len(rounds):
            greet(hello.at[at + 1], rounds[at + 1])

    for n in range(len(rounds)):
        S.add(("spread", n), [("spread", n - 1)] if n else [], 0.05, functools.partial(spread, n),
              sends=(("hello", n), "hello", 2.5, 0.0), gets=("hello", n - 1) if n else ("at", 1.5))
    met_all = [("spread", len(rounds) - 1)]

    S.add("rhs here", [], 0.0, locs["rhs"].wait, gets=("at", 0.5))
    S.add("err here", [], 0.0, locs["err"].wait, gets=("at", 0.5))
    S.add("cof here", [], 0.0, locs["cof"].wait, gets=("at", 1.0))
    S.add("home", [], 0.0, locs["home"].wait, gets=("at", 9.0))
    S.add("rhs there", [], 0.01, arrivals[0].wait_recv, gets=("at", SWAP_START + SWAP_FIELD))

    def err_there():
        arrivals[1].wait_recv()
        swaps[3].start()
        pl.when(has_prev)(wn_copy.start)

    S.add("err there", ["err here"], 0.03, err_there, sends=("next weights", "weights", 4.8, 0.0),
          gets=("at", SWAP_START + 2 * SWAP_FIELD))
    S.add("next weights", [], 0.01, lambda: pl.when(has_next)(wn_copy.wait_recv), gets="next weights")
    S.add("diagonal", [], 0.6, diagonal, gets=("at", SWAP_START + 1.3 * SWAP_FIELD))

    def piece(n):
        arrivals[2 + n].wait_recv()
        if 4 + n < len(swaps):
            swaps[4 + n].start()

    for n, k in enumerate(pieces):
        S.add(("cof", k), ["cof here"], 0.02, functools.partial(piece, n),
              gets=("at", SWAP_START + SWAP_FIELD * (2 + 4.0 * (n + 1) / many)))

    def whole_rows(it, i, k):
        if it == 0:
            return ["rhs here", "rhs there"]
        return [("image", it - 1, i, k)]

    def edges_out(it, side):
        k, at = (0, 0) if side == 0 else (final, last)
        if it == 1:
            at = 0 if side == 0 else EDGE - 1
            for i in range(2):
                eo[it, side, i:i + 1] = image(0, i, k, alone=True)[at:at + 1]
        else:
            for i in range(2):
                eo[it, side, i:i + 1] = states[it][i, at:at + 1]
        pl.when(ways[side])(edge_copy(eo, ei, h_send, h_recv, it, side).start)

    def adjoint_out(it, side):
        at = 0 if side == 0 else last
        here = slice(at, at + 1)
        go[it, side, 0:1] = c[1, 0, here] * qb[it, here]
        go[it, side, 1:2] = c[1, 1, here] * qn[it, here]
        pl.when(ways[side])(edge_copy(go, gi, g_send, g_recv, it, side).start)

    def store_image(it, i, k):
        y[it, i, rowset(k)] = image(it, i, k)
        if i == 0 and it + 1 < ITERS:
            pl.when(has_prev)(back_copy(it + 1, k).start)

    for it in range(ITERS):
        for side, k in ((0, 0), (1, final)):
            if it == 1:
                needs = [("here", 0, k), ("next", 0, k), ("forth", 0, k), ("adjoint in", 0, side), "diagonal"]
            else:
                needs = whole_rows(it, 0, k) + whole_rows(it, 1, k)
            S.add(("edges out", it, side), needs, 0.12, functools.partial(edges_out, it, side),
                  sends=(("edges", it, side), ("tile", side), HOP, 0.1))
            S.add(("edges in", it, side), [], 0.02, lambda it=it, side=side: pl.when(ways[side])(
                edge_in(eo, ei, h_send, h_recv, it, side).wait_recv), gets=("edges", it, 1 - side))
            S.add(("adjoint out", it, side), [("here", it, k), ("next", it, k)], 0.06,
                  functools.partial(adjoint_out, it, side),
                  sends=(("adjoint", it, side), ("tile", side), HOP, 0.1))
            S.add(("adjoint in", it, side), [], 0.02, lambda it=it, side=side: pl.when(ways[side])(
                edge_in(go, gi, g_send, g_recv, it, side).wait_recv), gets=("adjoint", it, 1 - side))
        for k in range(blocks):
            if it == 0:
                S.add(("back out", 0, k), whole_rows(0, 0, k), 0.02,
                      lambda k=k: pl.when(has_prev)(back_copy(0, k).start),
                      sends=(("back", 0, k), "back", HOP, BLOCK))
            S.add(("back", it, k), [], 0.02, lambda it=it, k=k: pl.when(has_next)(
                back_copy(it, k).wait_recv), gets=("back", it, k))
            S.add(("forth", it, k), [], 0.02, lambda it=it, k=k: pl.when(has_prev)(
                forth_copy(it, k).wait_recv), gets=("forth", it, k))
            around = [m for m in (k - 1, k, k + 1) if 0 <= m < blocks]
            ends = [side for side, m in ((0, 0), (1, final)) if m == k]
            for i in range(2):
                needs = [("cof", k)] + [("edges in", it, side) for side in ends]
                for m in around:
                    needs += whole_rows(it, i, m)
                S.add(("model", it, i, k), needs, 0.05, functools.partial(model, it, i, k),
                      sends=(("forth", it, k), "forth", HOP, BLOCK) if i == 1 else None)
                needs = ["diagonal", "err here", "err there"] + [("adjoint in", it, side) for side in ends]
                needs += [("next" if i else "here", it, m) for m in around]
                needs += [("here", it, k)] if i else [("forth", it, k)]
                S.add(("image", it, i, k), needs, 0.06, functools.partial(store_image, it, i, k),
                      sends=(("back", it + 1, k), "back", HOP, BLOCK) if i == 0 and it + 1 < ITERS else None)
            S.add(("here", it, k), ["err here", "err there", ("model", it, 0, k)], 0.03,
                  functools.partial(misfit_here, it, k))
            S.add(("next", it, k), ["next weights", ("model", it, 1, k), ("back", it, k)], 0.03,
                  functools.partial(misfit_next, it, k))
            S.add(("ret out", it, k), [("image", it, 0, k), ("image", it, 1, k)], 0.02,
                  lambda it=it, k=k: ret_copy(it, k).start(),
                  sends=(("ret", it, k), "ret", HOP, BLOCK))
            S.add(("ret", it, k), [], 0.01, lambda it=it, k=k: ret_copy(it, k).wait_recv(),
                  gets=("ret", it, k))

    def images(it):
        return [("image", it, i, k) for i in range(2) for k in range(blocks)]

    def moment(n, a, b):
        early[n:n + 1] = lanes(a, b)

    S.add("moment 0", ["rhs here", "rhs there"], 0.15, lambda: moment(0, v, v))
    S.add("moment 1", images(0), 0.3, lambda: (moment(1, v, y.at[0]), moment(2, y.at[0], y.at[0])))
    S.add("moment 3", images(1), 0.3,
          lambda: (moment(3, y.at[0], y.at[1]), moment(4, y.at[1], y.at[1])))

    S.add("early out", ["moment 0", "moment 1", "moment 3"] + met_all, 0.4,
          lambda: to_all(early, reds, 0), sends=("early", "all", REDUCE, 0.0))

    def late_out():
        late[...] = lanes(y.at[1], y.at[2])
        to_all(late, lasts, 1)

    S.add("late out", images(2) + met_all, 0.5, late_out, sends=("late", "all", REDUCE, 0.0))

    def early_in():
        m = from_all(reds, 0)
        plain = jnp.sum(m[0], axis=1, keepdims=True)
        g0 = plain[0:1]
        a0 = g0 / plain[1:2]
        less = pair_add(pair_rows(m, 0, 4), pair_scale(pair_rows(m, 1, 5), -a0))
        less = pair_add(pair_rows(less, 0, 3), pair_scale(pair_rows(less, 1, 4), -a0))
        one = pair_total(less)
        g1, d1 = one[0:1], one[1:2]
        b1 = g1 / g0
        a1 = g1 / (d1 - b1 * g1 / a0)
        p1 = -(a0 + a1 + a1 * b1)
        p2 = a0 * a1
        q = pair_add(pair_add(pair_rows(m, 0, 3), pair_scale(pair_rows(m, 1, 4), p1)),
                     pair_scale(pair_rows(m, 2, 5), p2))
        g2 = pair_total(pair_add(pair_add(pair_rows(q, 0, 1), pair_scale(pair_rows(q, 1, 2), p1)),
                                 pair_scale(pair_rows(q, 2, 3), p2)))
        rest = pair_add(pair_rows(m, 3, 4), pair_scale(pair_rows(m, 4, 5), p1))
        base = pair_add(pair_add(pair_rows(q, 1, 2), pair_scale(pair_rows(q, 2, 3), p1)),
                        pair_scale(rest, p2))
        scalars.update(a0=a0, a1=a1, b1=b1, p1=p1, p2=p2, g2=g2, b2=g2 / g1, base=base)

    S.add("early in", [], 0.6, early_in, gets="early")

    def late_in():
        s = scalars
        m = from_all(lasts, 1)
        d2 = pair_total(pair_add(s["base"], pair_scale(pair_scale(m, s["p2"]), s["p2"])))
        scalars["a2"] = s["g2"] / (d2 - s["b2"] * s["g2"] / s["a1"])

    S.add("late in", ["early in"], 0.4, late_in, gets="late")

    def own(level):
        return lambda at: v[level, at], lambda it, at: y[it, level, at]

    def away():
        return lambda at: home[at], lambda it, at: rt[it, at]

    def solve(level, source, k):
        s = scalars
        at = rowset(k)
        first, images_of = source
        r0, y0, y1 = first(at), images_of(0, at), images_of(1, at)
        p = (r0 - s["a0"] * y0) + s["b1"] * r0
        r2 = (r0 + s["p1"] * y0) + s["p2"] * y1
        x_out[0, level, at] = s["a0"] * r0 + s["a1"] * p
        r_out[0, level, at] = r2
        step[level, at] = r2 + s["b2"] * p

    def tail(level, source, k):
        s = scalars
        at = rowset(k)
        _, images_of = source
        y0, y1, y2 = images_of(0, at), images_of(1, at), images_of(2, at)
        s1 = (y0 - s["a0"] * y1) + s["b1"] * y0
        grad[level, at] = ((y0 + s["p1"] * y1) + s["p2"] * y2) + s["b2"] * s1

    def finish(level, k):
        at = rowset(k)
        x_out[0, level, at] = x_out[0, level, at] + scalars["a2"] * step[level, at]
        r_out[0, level, at] = r_out[0, level, at] - scalars["a2"] * grad[level, at]

    for k in range(blocks):
        S.add(("solve own", k), ["early in"] + [("image", it, i, k) for it in range(2) for i in range(2)],
              0.06, functools.partial(solve, lev, own(lev), k))
        S.add(("solve away", k), ["early in", "home"] + [("ret", it, k) for it in range(2)],
              0.06, functools.partial(solve, other, away(), k))
        S.add(("tail own", k), ["early in"] + [("image", it, i, k) for it in range(3) for i in range(2)],
              0.06, functools.partial(tail, lev, own(lev), k))
        S.add(("tail away", k), ["early in"] + [("ret", it, k) for it in range(3)],
              0.06, functools.partial(tail, other, away(), k))
        S.add(("finish own", k), ["late in", ("solve own", k), ("tail own", k)],
              0.04, functools.partial(finish, lev, k))
        S.add(("finish away", k), ["late in", ("solve away", k), ("tail away", k)],
              0.04, functools.partial(finish, other, k))

    order = S.order()
    if SHOW:
        for name, _, when in order:
            print(f"{when:6.2f}", name)
    for name, run, _ in order:
        run()

    for one in swaps:
        one.wait_send()
    ob_copy.wait_send()
    pl.when(has_prev)(wn_copy.wait_send)
    for it in range(ITERS):
        for side in range(2):
            pl.when(ways[side])(edge_copy(eo, ei, h_send, h_recv, it, side).wait_send)
            pl.when(ways[side])(edge_copy(go, gi, g_send, g_recv, it, side).wait_send)
        for k in range(blocks):
            ret_copy(it, k).wait_send()

        @pl.when(has_prev)
        def _():
            for k in range(blocks):
                back_copy(it, k).wait_send()

        @pl.when(has_next)
        def _():
            for k in range(blocks):
                forth_copy(it, k).wait_send()

    for sems, into in ((0, reds), (1, lasts)):
        most = into.at[pl.ds(0, count - 1)]
        pltpu.make_async_copy(most, most, rd_send.at[sems]).wait()


SHOW = False


def on_device(wins, tiles, right_side, error_weight, coeffs, obs_block, obs_pos, obs_weight):
    _, levels, rows, cols = right_side.shape
    nblk, width = obs_pos.shape[1:]
    f32 = jnp.float32
    vm = functools.partial(pltpu.VMEM, dtype=f32)
    dma = pltpu.SemaphoreType.DMA
    hbm = pl.BlockSpec(memory_space=pltpu.HBM)
    vmem = pl.BlockSpec(memory_space=pltpu.VMEM)
    blocks = rows // EDGE
    field = (rows, cols)
    edge = vm((ITERS, 2, 2, cols))
    scratch = [
        pltpu.VMEM(obs_block.shape, jnp.int32),
        pltpu.VMEM(obs_pos.shape, jnp.int32),
        vm(obs_weight.shape),
        vm((2,) + field),
        vm((ITERS, 2) + field),
        vm((2,) + field),
        vm(field),
        vm((4, 2) + field),
        vm((2,) + field),
        vm((2, nblk + 8, width)),
        vm((ITERS, 2) + field),
        vm((ITERS,) + field),
        vm((ITERS,) + field),
        vm((ITERS,) + field),
        vm((ITERS,) + field),
        edge, edge, edge, edge,
        vm((ITERS,) + field),
        vm(field),
        vm((2,) + field),
        vm((2,) + field),
        vm((MOMENTS, width)),
        vm((1, width)),
        vm((wins * tiles, MOMENTS, width)),
        vm((wins * tiles, 1, width)),
        dma((3 + blocks,)), dma((3 + blocks,)), dma((7,)),
        dma((ITERS, 2)), dma((ITERS, 2)),
        dma((2, ITERS, blocks)), dma((2, ITERS, blocks)),
        dma((ITERS, 2)), dma((ITERS, 2)),
        dma((ITERS, blocks)), dma((ITERS, blocks)),
        dma((2,)), dma((2,)),
        dma, dma,
        pltpu.SemaphoreType.REGULAR((1 + len(doubling(tiles)) + len(doubling(wins // 2)),)),
    ]
    out = vm(right_side.shape)
    return pl.pallas_call(
        functools.partial(kernel, wins, tiles),
        out_shape=(out, out),
        in_specs=[hbm] * 6,
        out_specs=(vmem, vmem),
        scratch_shapes=scratch,
        compiler_params=pltpu.CompilerParams(has_side_effects=True, collective_id=0,
                                             vmem_limit_bytes=60 * 1024 * 1024),
    )(right_side, error_weight, coeffs, obs_block, obs_pos, obs_weight)


def solution(mesh):
    in_specs = (
        P("win", None, "tile", None),
        P("win", None, "tile", None),
        P(None, "win", None, "tile", None),
        P("win", "tile"),
        P("win", "tile", None),
        P("win", "tile", None),
    )
    out_specs = (P("win", None, "tile", None), P("win", None, "tile", None))
    return jax.shard_map(
        functools.partial(on_device, mesh.shape["win"], mesh.shape["tile"]),
        mesh=mesh, in_specs=in_specs, out_specs=out_specs, check_vma=False
    )
```

```python
import functools

import jax
import jax.numpy as jnp
from jax import lax
from jax.experimental import pallas as pl
from jax.experimental.pallas import tpu as pltpu
from jax.sharding import PartitionSpec as P

ITERS = 3
EDGE = 8
MOMENTS = 2 * ITERS - 1

HOP, TILE_HOPS, BLOCK, SWAP_START, SWAP_FIELD, REDUCE, BEGIN = 2.2, (2.8, 1.5), 0.7, 2.2, 2.83, 5.2, 7.5


def doubling(length):
    steps, known = [], 1
    while known < length - 1:
        steps.append(known)
        known *= 2
    return steps


class Steps:
    def __init__(self):
        self.todo = {}

    def add(self, name, needs, cost, run, sends=None, gets=None):
        self.todo[name] = (list(needs), cost, run, sends, gets)

    def order(self):
        senders = {sends[0]: name for name, (_, _, _, sends, _) in self.todo.items() if sends}
        after = {name: [] for name in self.todo}
        for name, (needs, _, _, _, gets) in self.todo.items():
            for need in needs:
                after[need].append((name, 0.0))
            if gets in senders:
                after[senders[gets]].append((name, self.todo[senders[gets]][3][2]))
        rank = {}

        def path(name):
            if name not in rank:
                rank[name] = self.todo[name][1] + max(
                    (wait + path(then) for then, wait in after[name]), default=0.0)
            return rank[name]

        for name in self.todo:
            path(name)
        now, done, arrive, free, result = BEGIN, set(), {}, {}, []
        for _, (_, _, _, _, gets) in self.todo.items():
            if isinstance(gets, tuple) and gets[0] == "at":
                arrive[gets] = gets[1]
        left = dict(self.todo)
        while left:
            ready, soon = None, None
            for name, (needs, _, _, _, gets) in left.items():
                if any(need not in done for need in needs):
                    continue
                at = arrive.get(gets, None) if gets is not None else 0.0
                if at is None:
                    continue
                if at <= now:
                    if ready is None or rank[name] > rank[ready]:
                        ready = name
                elif soon is None or at < soon[0]:
                    soon = (at, name)
            pick = ready
            if pick is None:
                now, pick = soon
            _, cost, run, sends, _ = left.pop(pick)
            now += cost
            done.add(pick)
            if sends:
                message, link, latency, busy = sends
                begin = max(now, free.get(link, 0.0))
                free[link] = begin + busy
                arrive[message] = begin + busy + latency
            result.append((pick, run, now))
        return result


def two_sum(a, b):
    total = a + b
    back = total - a
    return total, (a - (total - back)) + (b - back)


def halves(a):
    big = 4097.0 * a
    high = big - (big - a)
    return high, a - high


def two_product(a, b):
    (ah, al), (bh, bl) = halves(a), halves(b)
    product = a * b
    return product, ((ah * bh - product) + ah * bl + al * bh) + al * bl


def pair_add(a, b):
    total, rest = two_sum(a[0], b[0])
    rest = rest + (a[1] + b[1])
    high = total + rest
    return high, rest - (high - total)


def pair_scale(a, factor):
    product, rest = two_product(a[0], factor)
    rest = rest + a[1] * factor
    high = product + rest
    return high, rest - (high - product)


def pair_rows(a, lo, hi):
    return a[0][lo:hi], a[1][lo:hi]


def pair_total(a):
    return jnp.sum(a[0], axis=1, keepdims=True) + jnp.sum(a[1], axis=1, keepdims=True)


def kernel(wins, tiles, rhs, err, cof, oblk_in, opos_in, owgt_in, x_out, r_out,
           obk, ops, owt, v, y, w, wn, c, d, ob, u, ui, vn, qb, qn, eo, ei, go, gi, rt, home,
           step, grad, energy, early, late, reds, lasts,
           x_sem, xs_sem, l_sem, h_send, h_recv, b_send, b_recv, g_send, g_recv,
           rt_send, rt_recv, rd_send, rd_recv, wn_send, wn_recv, hello):
    me_w = lax.axis_index("win")
    me_t = lax.axis_index("tile")
    lev = lax.rem(me_w, 2)
    other = 1 - lev
    mate = me_w + 1 - 2 * lev
    has_next = me_w + 2 < wins
    has_prev = me_w >= 2
    rows, cols = v.shape[1], v.shape[2]
    count = wins * tiles
    me = me_w * tiles + me_t
    width = ops.shape[2]
    nblk = ops.shape[1]
    last = rows - 1
    blocks = rows // EDGE
    final = blocks - 1
    pieces = list(range(final - 1)) + [final, final - 1]
    many = len(pieces)
    f32 = jnp.float32

    odd = lax.rem(me_t, 2)
    even = odd == 0

    def first_row(k):
        return pl.multiple_of((k + odd * (final - 2 * k)) * EDGE, EDGE)

    def rowset(k):
        return pl.ds(first_row(k), EDGE)

    def row_beyond(k, side):
        return pl.ds(first_row(k) - 1 + 9 * odd if side == 0 else first_row(k) + EDGE - 9 * odd, 1)

    def edge_row(side):
        return pl.ds(odd * last if side == 0 else last - odd * last, 1)

    beside = (me_t - 1 + 2 * odd, me_t + 1 - 2 * odd)
    ways = tuple(jnp.logical_and(tile >= 0, tile < tiles) for tile in beside)

    def remote(src, dst, ssem, rsem, win, tile):
        return pltpu.make_async_remote_copy(
            src_ref=src, dst_ref=dst, send_sem=ssem, recv_sem=rsem,
            device_id=(win, tile), device_id_type=pl.DeviceIdType.MESH)

    barrier = pltpu.get_barrier_semaphore()

    def signal(sem, win, tile):
        pl.semaphore_signal(sem, inc=1, device_id=(win, tile), device_id_type=pl.DeviceIdType.MESH)

    def greet(sem, ends):
        for there, win, tile in ends:
            pl.when(there)(functools.partial(signal, sem, win, tile))

    def met(sem, ends):
        pl.semaphore_wait(sem, sum(there.astype(jnp.int32) for there, _, _ in ends))

    def along_tile(hop):
        return [(me_t >= hop, me_w, me_t - hop), (me_t + hop < tiles, me_w, me_t + hop)]

    def along_win(hop):
        return [(me_w >= 2 * hop, me_w - 2 * hop, me_t),
                (me_w + 2 * hop < wins, me_w + 2 * hop, me_t)]

    facing = [(me_w >= 0, mate, me_t)]
    near = facing + along_tile(1) + along_win(1)
    rounds = ([along_tile(hop) for hop in doubling(tiles)] + [facing]
              + [along_win(hop) for hop in doubling(wins // 2)])

    greet(barrier, near)

    swaps = [
        remote(rhs.at[0, other], v.at[lev], xs_sem.at[0], x_sem.at[0], mate, me_t),
        remote(err.at[0, other], w.at[lev], xs_sem.at[1], x_sem.at[1], mate, me_t),
    ] + [
        remote(cof.at[:, 0, other, rowset(k)], c.at[:, lev, rowset(k)],
               xs_sem.at[3 + n], x_sem.at[3 + n], mate, me_t)
        for n, k in enumerate(pieces)
    ]
    arrivals = [
        remote(rhs.at[0, other], v.at[other], xs_sem.at[0], x_sem.at[0], mate, me_t),
        remote(err.at[0, other], w.at[other], xs_sem.at[1], x_sem.at[1], mate, me_t),
    ] + [
        remote(cof.at[:, 0, other, rowset(k)], c.at[:, other, rowset(k)],
               xs_sem.at[3 + n], x_sem.at[3 + n], mate, me_t)
        for n, k in enumerate(pieces)
    ]
    locs = {
        "block": pltpu.make_async_copy(oblk_in, obk, l_sem.at[4]),
        "pos": pltpu.make_async_copy(opos_in, ops, l_sem.at[5]),
        "weight": pltpu.make_async_copy(owgt_in, owt, l_sem.at[6]),
        "rhs": pltpu.make_async_copy(rhs.at[0, lev], v.at[lev], l_sem.at[0]),
        "err": pltpu.make_async_copy(err.at[0, lev], w.at[lev], l_sem.at[1]),
        "home": pltpu.make_async_copy(rhs.at[0, other], home, l_sem.at[2]),
        "cof": pltpu.make_async_copy(cof.at[:, 0, lev], c.at[:, lev], l_sem.at[3]),
    }
    for one in locs.values():
        one.start()
    met(barrier, near)
    for one in swaps[:3]:
        one.start()
    greet(hello.at[0], rounds[0])

    for side in range(2):
        @pl.when(jnp.logical_not(ways[side]))
        def _():
            for it in range(ITERS):
                ei[it, side] = jnp.zeros(ei.shape[2:], f32)
                gi[it, side] = jnp.zeros(gi.shape[2:], f32)

    @pl.when(jnp.logical_not(has_prev))
    def _():
        for it in range(ITERS):
            ui[it] = jnp.zeros(ui.shape[1:], f32)

    @pl.when(jnp.logical_not(has_next))
    def _():
        wn[...] = jnp.zeros(wn.shape, f32)
        for it in range(ITERS):
            vn[it] = jnp.zeros(vn.shape[1:], f32)

    states = (v, y.at[0], y.at[1])
    row8 = lax.broadcasted_iota(jnp.int32, (EDGE, cols), 0)

    def east(a):
        return pltpu.roll(a, cols - 1, 1)

    def west(a):
        return pltpu.roll(a, 1, 1)

    def sides(a, beyond):
        top, bottom = jnp.where(even, beyond[0], beyond[1]), jnp.where(even, beyond[1], beyond[0])
        return (jnp.where(row8 == 0, top, pltpu.roll(a, 1, 0))
                + jnp.where(row8 == EDGE - 1, bottom, pltpu.roll(a, EDGE - 1, 0)))

    def edge_copy(out, into, ssem, rsem, it, side, i):
        return remote(out.at[it, side, i], into.at[it, side, i], ssem.at[it, side, i],
                      rsem.at[it, side, i], me_w, beside[side])

    def back_copy(it, k):
        return remote(states[it].at[0, rowset(k)], vn.at[it, rowset(k)],
                      b_send.at[0, it, k], b_recv.at[0, it, k], me_w - 2, me_t)

    def forth_copy(it, k):
        return remote(u.at[it, 1, rowset(k)], ui.at[it, rowset(k)],
                      b_send.at[1, it, k], b_recv.at[1, it, k], me_w + 2, me_t)

    def ret_copy(it, k):
        return remote(y.at[it, other, rowset(k)], rt.at[it, rowset(k)],
                      rt_send.at[it, k], rt_recv.at[it, k], mate, me_t)

    wn_copy = remote(w.at[0], wn, wn_send, wn_recv, me_w - 2, me_t)

    def end_side(k):
        return 0 if k == 0 else 1 if k == final else None

    def model(it, i, k):
        src, at = states[it], rowset(k)
        a = src[i, at]
        beyond = [ei[it, side, i] if side == end_side(k) else src[i, row_beyond(k, side)]
                  for side in range(2)]
        u[it, i, at] = (c[0, i, at] * a + c[1, i, at] * sides(a, beyond)
                        + c[2, i, at] * east(a) + c[3, i, at] * west(a))
        if i == 1:
            pl.when(has_next)(forth_copy(it, k).start)

    def misfit_here(it, k):
        at = rowset(k)
        qb[it, at] = w[1, at] * (states[it][1, at] - u[it, 0, at])

    def misfit_next(it, k):
        at = rowset(k)
        qn[it, at] = wn[at] * (vn[it, at] - u[it, 1, at])

    def adjoint(it, i, q, k, alone=None):
        at = rowset(k)
        a = q[it, at]
        beyond = []
        for side in range(2):
            if side == end_side(k):
                beyond.append(gi[it, side, i])
            elif alone is not None:
                beyond.append(jnp.zeros((1, cols), f32))
            else:
                row = row_beyond(k, side)
                beyond.append(c[1, i, row] * q[it, row])
        return (c[0, i, at] * a + sides(c[1, i, at] * a, beyond)
                + west(c[2, i, at] * a) + east(c[3, i, at] * a))

    def image(it, i, k, alone=None):
        at = rowset(k)
        src = states[it]
        if i == 1:
            return (qb[it, at] + d[1, at] * src[1, at]) - adjoint(it, 1, qn, k, alone)
        return (d[0, at] * src[0, at] - adjoint(it, 0, qb, k, alone)) + w[0, at] * (src[0, at] - ui[it, at])

    def diagonal():
        ob_back.wait_recv()
        per_row = cols // width
        base = lev * (rows * per_row)
        spot = lax.broadcasted_iota(jnp.int32, (rows, nblk), 0) * per_row + base
        for i in range(2):
            who = ob[i, nblk:nblk + 1, 0:nblk]
            sums = ob[i, 0:nblk, :]
            for k in range(per_row):
                hot = jnp.where((spot + k).astype(f32) == who, 1.0, 0.0)
                d[i, :, k * width:(k + 1) * width] = jnp.dot(
                    hot, sums, precision=lax.Precision.HIGHEST, preferred_element_type=f32)

    def lanes(a, b):
        total = None
        for k in range(blocks):
            at = slice(k * EDGE, (k + 1) * EDGE)
            here = a[0, at] * b[0, at] + a[1, at] * b[1, at]
            total = here if total is None else total + here
        return folded(total)

    def folded(total):
        total = jnp.sum(total, axis=0, keepdims=True)
        parts = [total[:, k * width:(k + 1) * width] for k in range(cols // width)]
        while len(parts) > 1:
            parts = [sum(parts[k:k + 2]) for k in range(0, len(parts), 2)]
        return parts[0]

    def to_all(part, into, sems):
        turned = 2 * me < count

        def send(o, carry):
            to = lax.rem(me + jnp.where(turned, count - o, o), count)
            remote(part, into.at[me], rd_send.at[sems], rd_recv.at[sems],
                   to // tiles, lax.rem(to, tiles)).start()
            return carry

        lax.fori_loop(1, count, send, 0)
        into[me] = part[...]

    def from_all(into, sems):
        most = into.at[pl.ds(0, count - 1)]
        pltpu.make_async_copy(most, most, rd_recv.at[sems]).wait()
        high, low = into[0], jnp.zeros(into.shape[1:], f32)
        for k in range(1, count):
            high, rest = two_sum(high, into[k])
            low = low + rest
        return high, low

    def edges_out(it, side, i):
        if it == 0:
            eo[it, side, i] = v[i, edge_row(side)]
        else:
            whole = image(it - 1, i, 0 if side == 0 else final, alone=True)
            low, high = whole[0:1], whole[EDGE - 1:EDGE]
            eo[it, side, i] = jnp.where(even, low, high) if side == 0 else jnp.where(even, high, low)
        pl.when(ways[side])(edge_copy(eo, ei, h_send, h_recv, it, side, i).start)

    for one in ("block", "pos", "weight"):
        locs[one].wait()
    cell = lax.broadcasted_iota(jnp.int32, (width, width), 0)
    ones = jnp.ones((8, width), f32)
    ob[lev, nblk:, :] = jnp.zeros((8, width), f32)

    def per_block(b, carry):
        hit = jnp.where(cell == ops[0, pl.ds(b, 1), :], owt[0, pl.ds(b, 1), :], 0.0)
        total = lax.dot_general(ones, hit, (((1,), (1,)), ((), ())),
                                precision=lax.Precision.HIGHEST,
                                preferred_element_type=f32)
        ob[lev, pl.ds(b, 1), :] = total[0:1]
        return carry

    most = nblk - nblk // 4
    lax.fori_loop(0, most, per_block, 0)
    locs["rhs"].wait()
    arrivals[0].wait_recv()
    swaps[3].start()
    for k in range(blocks):
        pl.when(has_prev)(back_copy(0, k).start)
    for side in range(2):
        for i in range(2):
            edges_out(0, side, i)
    lax.fori_loop(most, nblk, per_block, 0)
    ob[lev, nblk:nblk + 1, 0:nblk] = obk[...].astype(f32)
    ob_copy = remote(ob.at[lev], ob.at[lev], xs_sem.at[2], x_sem.at[2], mate, me_t)
    ob_back = remote(ob.at[lev], ob.at[other], xs_sem.at[2], x_sem.at[2], mate, me_t)
    ob_copy.start()
    for one in swaps[4:]:
        one.start()

    S = Steps()
    scalars = {}

    def spread(at):
        met(hello.at[at], rounds[at])
        if at + 1 < len(rounds):
            greet(hello.at[at + 1], rounds[at + 1])

    for n in range(len(rounds)):
        S.add(("spread", n), [("spread", n - 1)] if n else [], 0.05, functools.partial(spread, n),
              sends=(("hello", n), "hello", 3.0, 0.0), gets=("hello", n - 1) if n else ("at", 1.5))
    met_all = [("spread", len(rounds) - 1)]

    S.add("err here", [], 0.0, locs["err"].wait, gets=("at", 0.5))
    S.add("cof here", [], 0.0, locs["cof"].wait, gets=("at", 1.0))
    S.add("home", [], 0.0, locs["home"].wait, gets=("at", 9.0))

    def err_there():
        arrivals[1].wait_recv()
        pl.when(has_prev)(wn_copy.start)

    S.add("err there", ["err here"], 0.03, err_there, sends=("next weights", "weights", 4.8, 0.0),
          gets=("at", SWAP_START + 2 * SWAP_FIELD))
    S.add("next weights", [], 0.01, lambda: pl.when(has_next)(wn_copy.wait_recv), gets="next weights")
    S.add("diagonal", [], 0.6, diagonal, gets=("at", 11.5))

    for n, k in enumerate(pieces):
        S.add(("cof", k), ["cof here"], 0.02, arrivals[2 + n].wait_recv,
              gets=("at", SWAP_START + SWAP_FIELD * (2 + 4.0 * (n + 1) / many)))

    def whole_rows(it, i, k):
        if it == 0:
            return []
        return [("image", it - 1, i, k)]

    def adjoint_out(it, side, i):
        row = edge_row(side)
        go[it, side, i] = c[1, i, row] * (qn if i else qb)[it, row]
        pl.when(ways[side])(edge_copy(go, gi, g_send, g_recv, it, side, i).start)

    def edges_in(out, into, ssem, rsem, it, side, i):
        pl.when(ways[side])(edge_copy(out, into, ssem, rsem, it, side, i).wait_recv)

    def store_image(it, i, k):
        y[it, i, rowset(k)] = image(it, i, k)
        if i == 0 and it + 1 < ITERS:
            pl.when(has_prev)(back_copy(it + 1, k).start)

    for it in range(ITERS):
        for side, k in ((0, 0), (1, final)):
            for i in range(2):
                if it > 0:
                    needs = [("here", it - 1, k), ("adjoint in", it - 1, side, i), "diagonal"]
                    needs += [("next", it - 1, k)] if i else [("forth", it - 1, k)]
                    S.add(("edges out", it, side, i), needs, 0.06, functools.partial(edges_out, it, side, i),
                          sends=(("edges", it, side, i), ("tile", side), TILE_HOPS[side], 0.05))
                S.add(("edges in", it, side, i), [], 0.02,
                      functools.partial(edges_in, eo, ei, h_send, h_recv, it, side, i),
                      gets=("edges", it, side, i) if it else ("at", 7.7))
                S.add(("adjoint out", it, side, i), [("next" if i else "here", it, k)], 0.03,
                      functools.partial(adjoint_out, it, side, i),
                      sends=(("adjoint", it, side, i), ("tile", side), TILE_HOPS[side], 0.05))
                S.add(("adjoint in", it, side, i), [], 0.02,
                      functools.partial(edges_in, go, gi, g_send, g_recv, it, side, i),
                      gets=("adjoint", it, side, i))
        for k in range(blocks):
            S.add(("back", it, k), [], 0.02, lambda it=it, k=k: pl.when(has_next)(
                back_copy(it, k).wait_recv),
                  gets=("back", it, k) if it else ("at", 8.0 + BLOCK * k))
            S.add(("forth", it, k), [], 0.02, lambda it=it, k=k: pl.when(has_prev)(
                forth_copy(it, k).wait_recv), gets=("forth", it, k))
            around = [m for m in (k - 1, k, k + 1) if 0 <= m < blocks]
            ends = [side for side, m in ((0, 0), (1, final)) if m == k]
            for i in range(2):
                needs = [("cof", k)] + [("edges in", it, side, i) for side in ends]
                for m in around:
                    needs += whole_rows(it, i, m)
                S.add(("model", it, i, k), needs, 0.05, functools.partial(model, it, i, k),
                      sends=(("forth", it, k), "forth", HOP, BLOCK) if i == 1 else None)
                needs = ["diagonal", "err here", "err there"] + [("adjoint in", it, side, i) for side in ends]
                needs += [("next" if i else "here", it, m) for m in around]
                needs += [("here", it, k)] if i else [("forth", it, k)]
                S.add(("image", it, i, k), needs, 0.06, functools.partial(store_image, it, i, k),
                      sends=(("back", it + 1, k), "back", HOP, BLOCK) if i == 0 and it + 1 < ITERS else None)
            S.add(("here", it, k), ["err here", "err there", ("model", it, 0, k)] + whole_rows(it, 1, k), 0.03,
                  functools.partial(misfit_here, it, k))
            S.add(("next", it, k), ["next weights", ("model", it, 1, k), ("back", it, k)], 0.03,
                  functools.partial(misfit_next, it, k))
            S.add(("ret out", it, k), [("image", it, 0, k), ("image", it, 1, k)], 0.02,
                  lambda it=it, k=k: ret_copy(it, k).start(),
                  sends=(("ret", it, k), "ret", HOP, BLOCK))
            S.add(("ret", it, k), ["early in"] if it < 2 else [], 0.01, lambda it=it, k=k: ret_copy(it, k).wait_recv(),
                  gets=("ret", it, k))

    def images(it):
        return [("image", it, i, k) for i in range(2) for k in range(blocks)]

    def moment(n, a, b):
        early[n:n + 1] = lanes(a, b)

    S.add("moment 0", [], 0.15, lambda: moment(0, v, v))
    S.add("moment 1", images(0), 0.3, lambda: (moment(1, v, y.at[0]), moment(2, y.at[0], y.at[0])))
    S.add("moment 3", images(1), 0.3,
          lambda: (moment(3, y.at[0], y.at[1]), moment(4, y.at[1], y.at[1])))

    S.add("early out", ["moment 0", "moment 1", "moment 3", *[("model", 2, 1, k) for k in range(blocks)]] + met_all, 0.4,
          lambda: to_all(early, reds, 0), sends=("early", "all", REDUCE, 0.0))

    def energy_states():
        total = None
        first = jnp.where(has_prev, 0.0, 1.0)
        for k in range(blocks):
            at = slice(k * EDGE, (k + 1) * EDGE)
            a, b = states[2][0, at], states[2][1, at]
            here = (d[0, at] + first * w[0, at]) * (a * a) + d[1, at] * (b * b)
            total = here if total is None else total + here
        energy[...] = total

    def energy_misfits(k):
        at = rowset(k)
        energy[...] += (qb[2, at] * (states[2][1, at] - u[2, 0, at])
                        + qn[2, at] * (vn[2, at] - u[2, 1, at]))

    def late_out():
        late[...] = folded(energy[...])
        to_all(late, lasts, 1)

    S.add("energy", images(1), 0.1, energy_states)
    for k in range(blocks):
        S.add(("energy", k), ["energy", ("here", 2, k), ("next", 2, k)], 0.04,
              functools.partial(energy_misfits, k))
    S.add("late out", [("energy", k) for k in range(blocks)] + met_all, 0.5, late_out,
          sends=("late", "all", REDUCE, 0.0))

    def early_in():
        m = from_all(reds, 0)
        plain = jnp.sum(m[0], axis=1, keepdims=True)
        g0 = plain[0:1]
        a0 = g0 / plain[1:2]
        less = pair_add(pair_rows(m, 0, 4), pair_scale(pair_rows(m, 1, 5), -a0))
        less = pair_add(pair_rows(less, 0, 3), pair_scale(pair_rows(less, 1, 4), -a0))
        one = pair_total(less)
        g1, d1 = one[0:1], one[1:2]
        b1 = g1 / g0
        a1 = g1 / (d1 - b1 * g1 / a0)
        p1 = -(a0 + a1 + a1 * b1)
        p2 = a0 * a1
        q = pair_add(pair_add(pair_rows(m, 0, 3), pair_scale(pair_rows(m, 1, 4), p1)),
                     pair_scale(pair_rows(m, 2, 5), p2))
        g2 = pair_total(pair_add(pair_add(pair_rows(q, 0, 1), pair_scale(pair_rows(q, 1, 2), p1)),
                                 pair_scale(pair_rows(q, 2, 3), p2)))
        rest = pair_add(pair_rows(m, 3, 4), pair_scale(pair_rows(m, 4, 5), p1))
        base = pair_add(pair_add(pair_rows(q, 1, 2), pair_scale(pair_rows(q, 2, 3), p1)),
                        pair_scale(rest, p2))
        scalars.update(a0=a0, a1=a1, b1=b1, p1=p1, p2=p2, g2=g2, b2=g2 / g1, base=base)

    S.add("early in", ["late out"], 0.6, early_in, gets="early")

    def late_in():
        s = scalars
        m = from_all(lasts, 1)
        d2 = pair_total(pair_add(s["base"], pair_scale(pair_scale(m, s["p2"]), s["p2"])))
        scalars["a2"] = s["g2"] / (d2 - s["b2"] * s["g2"] / s["a1"])

    S.add("late in", ["early in", "sent"], 0.4, late_in, gets="late")

    def own(level):
        return lambda at: v[level, at], lambda it, at: y[it, level, at]

    def away():
        return lambda at: home[at], lambda it, at: rt[it, at]

    def solve(level, source, k):
        s = scalars
        at = rowset(k)
        first, images_of = source
        r0, y0, y1 = first(at), images_of(0, at), images_of(1, at)
        p = (r0 - s["a0"] * y0) + s["b1"] * r0
        r2 = (r0 + s["p1"] * y0) + s["p2"] * y1
        x_out[0, level, at] = s["a0"] * r0 + s["a1"] * p
        r_out[0, level, at] = r2
        step[level, at] = r2 + s["b2"] * p

    def tail(level, source, k):
        s = scalars
        at = rowset(k)
        _, images_of = source
        y0, y1, y2 = images_of(0, at), images_of(1, at), images_of(2, at)
        s1 = (y0 - s["a0"] * y1) + s["b1"] * y0
        grad[level, at] = ((y0 + s["p1"] * y1) + s["p2"] * y2) + s["b2"] * s1

    def finish(level, k):
        at = rowset(k)
        x_out[0, level, at] = x_out[0, level, at] + scalars["a2"] * step[level, at]
        r_out[0, level, at] = r_out[0, level, at] - scalars["a2"] * grad[level, at]

    for k in range(blocks):
        S.add(("solve own", k), ["early in"] + [("image", it, i, k) for it in range(2) for i in range(2)],
              0.06, functools.partial(solve, lev, own(lev), k))
        S.add(("solve away", k), ["early in", "home"] + [("ret", it, k) for it in range(2)],
              0.06, functools.partial(solve, other, away(), k))
        S.add(("tail own", k), ["early in"] + [("image", it, i, k) for it in range(3) for i in range(2)],
              0.06, functools.partial(tail, lev, own(lev), k))
        S.add(("tail away", k), ["early in"] + [("ret", it, k) for it in range(3)],
              0.06, functools.partial(tail, other, away(), k))
        S.add(("finish own", k), ["late in", ("solve own", k), ("tail own", k)],
              0.04, functools.partial(finish, lev, k))
        S.add(("finish away", k), ["late in", ("solve away", k), ("tail away", k)],
              0.04, functools.partial(finish, other, k))

    def sent():
        for one in swaps:
            one.wait_send()
        ob_copy.wait_send()
        pl.when(has_prev)(wn_copy.wait_send)
        for it in range(ITERS):
            for side in range(2):
                for i in range(2):
                    pl.when(ways[side])(edge_copy(eo, ei, h_send, h_recv, it, side, i).wait_send)
                    pl.when(ways[side])(edge_copy(go, gi, g_send, g_recv, it, side, i).wait_send)
            for k in range(blocks):
                ret_copy(it, k).wait_send()

            @pl.when(has_prev)
            def _():
                for k in range(blocks):
                    back_copy(it, k).wait_send()

            @pl.when(has_next)
            def _():
                for k in range(blocks):
                    forth_copy(it, k).wait_send()
        most = reds.at[pl.ds(0, count - 1)]
        pltpu.make_async_copy(most, most, rd_send.at[0]).wait()

    S.add("sent", [("tail away", k) for k in range(blocks)], 0.5, sent)
    order = S.order()
    if SHOW:
        for name, _, when in order:
            print(f"{when:6.2f}", name)
    for name, run, _ in order:
        run()

    most = lasts.at[pl.ds(0, count - 1)]
    pltpu.make_async_copy(most, most, rd_send.at[1]).wait()


SHOW = False


def on_device(wins, tiles, right_side, error_weight, coeffs, obs_block, obs_pos, obs_weight):
    _, levels, rows, cols = right_side.shape
    nblk, width = obs_pos.shape[1:]
    f32 = jnp.float32
    vm = functools.partial(pltpu.VMEM, dtype=f32)
    dma = pltpu.SemaphoreType.DMA
    hbm = pl.BlockSpec(memory_space=pltpu.HBM)
    vmem = pl.BlockSpec(memory_space=pltpu.VMEM)
    blocks = rows // EDGE
    field = (rows, cols)
    edge = vm((ITERS, 2, 2, 1, cols))
    scratch = [
        pltpu.VMEM(obs_block.shape, jnp.int32),
        pltpu.VMEM(obs_pos.shape, jnp.int32),
        vm(obs_weight.shape),
        vm((2,) + field),
        vm((ITERS, 2) + field),
        vm((2,) + field),
        vm(field),
        vm((4, 2) + field),
        vm((2,) + field),
        vm((2, nblk + 8, width)),
        vm((ITERS, 2) + field),
        vm((ITERS,) + field),
        vm((ITERS,) + field),
        vm((ITERS,) + field),
        vm((ITERS,) + field),
        edge, edge, edge, edge,
        vm((ITERS,) + field),
        vm(field),
        vm((2,) + field),
        vm((2,) + field),
        vm((EDGE, cols)),
        vm((MOMENTS, width)),
        vm((1, width)),
        vm((wins * tiles, MOMENTS, width)),
        vm((wins * tiles, 1, width)),
        dma((3 + blocks,)), dma((3 + blocks,)), dma((7,)),
        dma((ITERS, 2, 2)), dma((ITERS, 2, 2)),
        dma((2, ITERS, blocks)), dma((2, ITERS, blocks)),
        dma((ITERS, 2, 2)), dma((ITERS, 2, 2)),
        dma((ITERS, blocks)), dma((ITERS, blocks)),
        dma((2,)), dma((2,)),
        dma, dma,
        pltpu.SemaphoreType.REGULAR((1 + len(doubling(tiles)) + len(doubling(wins // 2)),)),
    ]
    out = vm(right_side.shape)
    return pl.pallas_call(
        functools.partial(kernel, wins, tiles),
        out_shape=(out, out),
        in_specs=[hbm] * 6,
        out_specs=(vmem, vmem),
        scratch_shapes=scratch,
        compiler_params=pltpu.CompilerParams(has_side_effects=True, collective_id=0,
                                             vmem_limit_bytes=60 * 1024 * 1024),
    )(right_side, error_weight, coeffs, obs_block, obs_pos, obs_weight)


def solution(mesh):
    in_specs = (
        P("win", None, "tile", None),
        P("win", None, "tile", None),
        P(None, "win", None, "tile", None),
        P("win", "tile"),
        P("win", "tile", None),
        P("win", "tile", None),
    )
    out_specs = (P("win", None, "tile", None), P("win", None, "tile", None))
    return jax.shard_map(
        functools.partial(on_device, mesh.shape["win"], mesh.shape["tile"]),
        mesh=mesh, in_specs=in_specs, out_specs=out_specs, check_vma=False
    )
```

```python
import functools

import jax
import jax.numpy as jnp
from jax import lax
from jax.experimental import pallas as pl
from jax.experimental.pallas import tpu as pltpu
from jax.sharding import PartitionSpec as P

ITERS = 3
EDGE = 8
MOMENTS = 2 * ITERS - 1

HOP, TILE_HOPS, BLOCK, SWAP_START, SWAP_FIELD, REDUCE, BEGIN = 2.2, (2.8, 1.5), 0.7, 2.2, 2.83, 5.2, 7.5


def doubling(length):
    steps, known = [], 1
    while known < length - 1:
        steps.append(known)
        known *= 2
    return steps


class Steps:
    def __init__(self):
        self.todo = {}

    def add(self, name, needs, cost, run, sends=None, gets=None):
        self.todo[name] = (list(needs), cost, run, sends, gets)

    def order(self):
        senders = {sends[0]: name for name, (_, _, _, sends, _) in self.todo.items() if sends}
        after = {name: [] for name in self.todo}
        for name, (needs, _, _, _, gets) in self.todo.items():
            for need in needs:
                after[need].append((name, 0.0))
            if gets in senders:
                after[senders[gets]].append((name, self.todo[senders[gets]][3][2]))
        rank = {}

        def path(name):
            if name not in rank:
                rank[name] = self.todo[name][1] + max(
                    (wait + path(then) for then, wait in after[name]), default=0.0)
            return rank[name]

        for name in self.todo:
            path(name)
        now, done, arrive, free, result = BEGIN, set(), {}, {}, []
        for _, (_, _, _, _, gets) in self.todo.items():
            if isinstance(gets, tuple) and gets[0] == "at":
                arrive[gets] = gets[1]
        left = dict(self.todo)
        while left:
            ready, soon = None, None
            for name, (needs, _, _, _, gets) in left.items():
                if any(need not in done for need in needs):
                    continue
                at = arrive.get(gets, None) if gets is not None else 0.0
                if at is None:
                    continue
                if at <= now:
                    if ready is None or rank[name] > rank[ready]:
                        ready = name
                elif soon is None or at < soon[0]:
                    soon = (at, name)
            pick = ready
            if pick is None:
                now, pick = soon
            _, cost, run, sends, _ = left.pop(pick)
            now += cost
            done.add(pick)
            if sends:
                message, link, latency, busy = sends
                begin = max(now, free.get(link, 0.0))
                free[link] = begin + busy
                arrive[message] = begin + busy + latency
            result.append((pick, run, now))
        return result


def two_sum(a, b):
    total = a + b
    back = total - a
    return total, (a - (total - back)) + (b - back)


def halves(a):
    big = 4097.0 * a
    high = big - (big - a)
    return high, a - high


def two_product(a, b):
    (ah, al), (bh, bl) = halves(a), halves(b)
    product = a * b
    return product, ((ah * bh - product) + ah * bl + al * bh) + al * bl


def pair_add(a, b):
    total, rest = two_sum(a[0], b[0])
    rest = rest + (a[1] + b[1])
    high = total + rest
    return high, rest - (high - total)


def pair_scale(a, factor):
    product, rest = two_product(a[0], factor)
    rest = rest + a[1] * factor
    high = product + rest
    return high, rest - (high - product)


def pair_rows(a, lo, hi):
    return a[0][lo:hi], a[1][lo:hi]


def pair_total(a):
    return jnp.sum(a[0], axis=1, keepdims=True) + jnp.sum(a[1], axis=1, keepdims=True)


def kernel(wins, tiles, rhs, err, cof, oblk_in, opos_in, owgt_in, x_out, r_out,
           obk, ops, owt, v, y, w, wn, c, d, ob, u, ui, vn, qb, qn, eo, ei, go, gi, rt, home,
           step, grad, energy, early, late, reds, lasts,
           x_sem, xs_sem, l_sem, f_recv, h_send, h_recv, b_send, b_recv, c_recv, g_send, g_recv,
           rt_send, rt_recv, rd_send, rd_recv, wn_send, wn_recv, hello):
    me_w = lax.axis_index("win")
    me_t = lax.axis_index("tile")
    lev = lax.rem(me_w, 2)
    other = 1 - lev
    mate = me_w + 1 - 2 * lev
    has_next = me_w + 2 < wins
    has_prev = me_w >= 2
    rows, cols = v.shape[1], v.shape[2]
    count = wins * tiles
    me = me_w * tiles + me_t
    width = ops.shape[2]
    nblk = ops.shape[1]
    last = rows - 1
    blocks = rows // EDGE
    final = blocks - 1
    pieces = list(range(final - 1)) + [final, final - 1]
    many = len(pieces)
    f32 = jnp.float32

    odd = lax.rem(me_t, 2)
    even = odd == 0

    def first_row(k):
        return pl.multiple_of((k + odd * (final - 2 * k)) * EDGE, EDGE)

    def rowset(k):
        return pl.ds(first_row(k), EDGE)

    def row_beyond(k, side):
        return pl.ds(first_row(k) - 1 + 9 * odd if side == 0 else first_row(k) + EDGE - 9 * odd, 1)

    def edge_row(side):
        return pl.ds(odd * last if side == 0 else last - odd * last, 1)

    beside = (me_t - 1 + 2 * odd, me_t + 1 - 2 * odd)
    ways = tuple(jnp.logical_and(tile >= 0, tile < tiles) for tile in beside)

    def remote(src, dst, ssem, rsem, win, tile):
        return pltpu.make_async_remote_copy(
            src_ref=src, dst_ref=dst, send_sem=ssem, recv_sem=rsem,
            device_id=(win, tile), device_id_type=pl.DeviceIdType.MESH)

    def all_of(ref, sem):
        return pltpu.make_async_copy(ref, ref, sem)

    barrier = pltpu.get_barrier_semaphore()

    def signal(sem, win, tile):
        pl.semaphore_signal(sem, inc=1, device_id=(win, tile), device_id_type=pl.DeviceIdType.MESH)

    def greet(sem, ends):
        for there, win, tile in ends:
            pl.when(there)(functools.partial(signal, sem, win, tile))

    def met(sem, ends):
        pl.semaphore_wait(sem, sum(there.astype(jnp.int32) for there, _, _ in ends))

    def along_tile(hop):
        return [(me_t >= hop, me_w, me_t - hop), (me_t + hop < tiles, me_w, me_t + hop)]

    def along_win(hop):
        return [(me_w >= 2 * hop, me_w - 2 * hop, me_t),
                (me_w + 2 * hop < wins, me_w + 2 * hop, me_t)]

    facing = [(me_w >= 0, mate, me_t)]
    near = facing + along_tile(1) + along_win(1)
    rounds = ([along_tile(hop) for hop in doubling(tiles)] + [facing]
              + [along_win(hop) for hop in doubling(wins // 2)])

    greet(barrier, near)

    swaps = [
        remote(rhs.at[0, other], v.at[lev], xs_sem.at[0], x_sem.at[0], mate, me_t),
        remote(err.at[0, other], w.at[lev], xs_sem.at[0], x_sem.at[1], mate, me_t),
    ] + [
        remote(cof.at[:, 0, other, rowset(k)], c.at[:, lev, rowset(k)],
               xs_sem.at[0], x_sem.at[3 + n], mate, me_t)
        for n, k in enumerate(pieces)
    ]
    arrivals = [
        remote(rhs.at[0, other], v.at[other], xs_sem.at[0], x_sem.at[0], mate, me_t),
        remote(err.at[0, other], w.at[other], xs_sem.at[0], x_sem.at[1], mate, me_t),
    ] + [
        remote(cof.at[:, 0, other, rowset(k)], c.at[:, other, rowset(k)],
               xs_sem.at[0], x_sem.at[3 + n], mate, me_t)
        for n, k in enumerate(pieces)
    ]
    locs = {
        "block": pltpu.make_async_copy(oblk_in, obk, l_sem.at[0]),
        "pos": pltpu.make_async_copy(opos_in, ops, l_sem.at[1]),
        "weight": pltpu.make_async_copy(owgt_in, owt, l_sem.at[4]),
        "rhs": pltpu.make_async_copy(rhs.at[0, lev], v.at[lev], l_sem.at[2]),
        "err": pltpu.make_async_copy(err.at[0, lev], w.at[lev], l_sem.at[3]),
        "home": pltpu.make_async_copy(rhs.at[0, other], home, l_sem.at[3]),
        "cof": pltpu.make_async_copy(cof.at[:, 0, lev], c.at[:, lev], l_sem.at[3]),
    }
    for one in locs.values():
        one.start()
    met(barrier, near)
    for one in swaps[:3]:
        one.start()
    greet(hello.at[0], rounds[0])

    for side in range(2):
        @pl.when(jnp.logical_not(ways[side]))
        def _():
            for it in range(ITERS):
                ei[it, side] = jnp.zeros(ei.shape[2:], f32)
                gi[it, side] = jnp.zeros(gi.shape[2:], f32)

    @pl.when(jnp.logical_not(has_prev))
    def _():
        for it in range(ITERS):
            ui[it] = jnp.zeros(ui.shape[1:], f32)

    @pl.when(jnp.logical_not(has_next))
    def _():
        wn[...] = jnp.zeros(wn.shape, f32)
        for it in range(ITERS):
            vn[it] = jnp.zeros(vn.shape[1:], f32)

    states = (v, y.at[0], y.at[1])
    row8 = lax.broadcasted_iota(jnp.int32, (EDGE, cols), 0)

    def east(a):
        return pltpu.roll(a, cols - 1, 1)

    def west(a):
        return pltpu.roll(a, 1, 1)

    def sides(a, beyond):
        top, bottom = jnp.where(even, beyond[0], beyond[1]), jnp.where(even, beyond[1], beyond[0])
        return (jnp.where(row8 == 0, top, pltpu.roll(a, 1, 0))
                + jnp.where(row8 == EDGE - 1, bottom, pltpu.roll(a, EDGE - 1, 0)))

    def edge_copy(out, into, ssem, rsem, it, side, i):
        return remote(out.at[it, side, i], into.at[it, side, i], ssem.at[side],
                      rsem(it, side, i), me_w, beside[side])

    def edge_sem(it, side, i):
        return f_recv.at[side] if it == 0 else h_recv.at[it - 1, side, i]

    def adjoint_sem(it, side, i):
        return g_recv.at[it, side, i]


    def back_copy(it, k):
        return remote(states[it].at[0, rowset(k)], vn.at[it, rowset(k)],
                      b_send.at[0], b_recv.at[it - 1, k] if it else f_recv.at[2], me_w - 2, me_t)

    def forth_copy(it, k):
        return remote(u.at[it, 1, rowset(k)], ui.at[it, rowset(k)],
                      b_send.at[1], c_recv.at[it, k], me_w + 2, me_t)

    def ret_copy(it, k):
        return remote(y.at[it, other, rowset(k)], rt.at[it, rowset(k)],
                      rt_send, rt_recv.at[k if it == ITERS - 1 else blocks], mate, me_t)

    wn_copy = remote(w.at[0], wn, wn_send, wn_recv, me_w - 2, me_t)

    def end_side(k):
        return 0 if k == 0 else 1 if k == final else None

    def model(it, i, k):
        src, at = states[it], rowset(k)
        a = src[i, at]
        beyond = [ei[it, side, i] if side == end_side(k) else src[i, row_beyond(k, side)]
                  for side in range(2)]
        u[it, i, at] = (c[0, i, at] * a + c[1, i, at] * sides(a, beyond)
                        + c[2, i, at] * east(a) + c[3, i, at] * west(a))
        if i == 1:
            pl.when(has_next)(forth_copy(it, k).start)

    def misfit_here(it, k):
        at = rowset(k)
        qb[it, at] = w[1, at] * (states[it][1, at] - u[it, 0, at])

    def misfit_next(it, k):
        at = rowset(k)
        qn[it, at] = wn[at] * (vn[it, at] - u[it, 1, at])

    def adjoint(it, i, q, k, alone=None):
        at = rowset(k)
        a = q[it, at]
        beyond = []
        for side in range(2):
            if side == end_side(k):
                beyond.append(gi[it, side, i])
            elif alone is not None:
                beyond.append(jnp.zeros((1, cols), f32))
            else:
                row = row_beyond(k, side)
                beyond.append(c[1, i, row] * q[it, row])
        return (c[0, i, at] * a + sides(c[1, i, at] * a, beyond)
                + west(c[2, i, at] * a) + east(c[3, i, at] * a))

    def image(it, i, k, alone=None):
        at = rowset(k)
        src = states[it]
        if i == 1:
            return (qb[it, at] + d[1, at] * src[1, at]) - adjoint(it, 1, qn, k, alone)
        return (d[0, at] * src[0, at] - adjoint(it, 0, qb, k, alone)) + w[0, at] * (src[0, at] - ui[it, at])

    def diagonal():
        ob_back.wait_recv()
        per_row = cols // width
        base = lev * (rows * per_row)
        spot = lax.broadcasted_iota(jnp.int32, (rows, nblk), 0) * per_row + base
        for i in range(2):
            who = ob[i, nblk:nblk + 1, 0:nblk]
            sums = ob[i, 0:nblk, :]
            for k in range(per_row):
                hot = jnp.where((spot + k).astype(f32) == who, 1.0, 0.0)
                d[i, :, k * width:(k + 1) * width] = jnp.dot(
                    hot, sums, precision=lax.Precision.HIGHEST, preferred_element_type=f32)

    def lanes(a, b):
        total = None
        for k in range(blocks):
            at = slice(k * EDGE, (k + 1) * EDGE)
            here = a[0, at] * b[0, at] + a[1, at] * b[1, at]
            total = here if total is None else total + here
        return folded(total)

    def folded(total):
        total = jnp.sum(total, axis=0, keepdims=True)
        parts = [total[:, k * width:(k + 1) * width] for k in range(cols // width)]
        while len(parts) > 1:
            parts = [sum(parts[k:k + 2]) for k in range(0, len(parts), 2)]
        return parts[0]

    def to_all(part, into, sems):
        turned = 2 * me < count

        def send(o, carry):
            to = lax.rem(me + jnp.where(turned, count - o, o), count)
            remote(part, into.at[me], rd_send.at[sems], rd_recv.at[sems],
                   to // tiles, lax.rem(to, tiles)).start()
            return carry

        lax.fori_loop(1, count, send, 0)
        into[me] = part[...]

    def from_all(into, sems):
        most = into.at[pl.ds(0, count - 1)]
        pltpu.make_async_copy(most, most, rd_recv.at[sems]).wait()
        high, low = into[0], jnp.zeros(into.shape[1:], f32)
        for k in range(1, count):
            high, rest = two_sum(high, into[k])
            low = low + rest
        return high, low

    def edges_out(it, side, i):
        if it == 0:
            eo[it, side, i] = v[i, edge_row(side)]
        else:
            whole = image(it - 1, i, 0 if side == 0 else final, alone=True)
            low, high = whole[0:1], whole[EDGE - 1:EDGE]
            eo[it, side, i] = jnp.where(even, low, high) if side == 0 else jnp.where(even, high, low)
        pl.when(ways[side])(edge_copy(eo, ei, h_send, edge_sem, it, side, i).start)

    for one in ("block", "pos", "weight"):
        locs[one].wait()
    cell = lax.broadcasted_iota(jnp.int32, (width, width), 0)
    ones = jnp.ones((8, width), f32)
    ob[lev, nblk:, :] = jnp.zeros((8, width), f32)

    def per_block(b, carry):
        hit = jnp.where(cell == ops[0, pl.ds(b, 1), :], owt[0, pl.ds(b, 1), :], 0.0)
        total = lax.dot_general(ones, hit, (((1,), (1,)), ((), ())),
                                precision=lax.Precision.HIGHEST,
                                preferred_element_type=f32)
        ob[lev, pl.ds(b, 1), :] = total[0:1]
        return carry

    most = nblk - nblk // 4
    lax.fori_loop(0, most, per_block, 0)
    locs["rhs"].wait()
    arrivals[0].wait_recv()
    swaps[3].start()
    for k in range(blocks):
        pl.when(has_prev)(back_copy(0, k).start)
    for side in range(2):
        for i in range(2):
            edges_out(0, side, i)
    lax.fori_loop(most, nblk, per_block, 0)
    ob[lev, nblk:nblk + 1, 0:nblk] = obk[...].astype(f32)
    ob_copy = remote(ob.at[lev], ob.at[lev], xs_sem.at[1], x_sem.at[2], mate, me_t)
    ob_back = remote(ob.at[lev], ob.at[other], xs_sem.at[1], x_sem.at[2], mate, me_t)
    ob_copy.start()
    for one in swaps[4:]:
        one.start()

    S = Steps()
    scalars = {}

    def spread(at):
        met(hello.at[at], rounds[at])
        if at + 1 < len(rounds):
            greet(hello.at[at + 1], rounds[at + 1])

    for n in range(len(rounds)):
        S.add(("spread", n), [("spread", n - 1)] if n else [], 0.05, functools.partial(spread, n),
              sends=(("hello", n), "hello", 3.0, 0.0), gets=("hello", n - 1) if n else ("at", 1.5))
    met_all = [("spread", len(rounds) - 1)]

    S.add("here", [], 0.01, all_of(y, l_sem.at[3]).wait, gets=("at", 1.0))

    def err_there():
        arrivals[1].wait_recv()
        pl.when(has_prev)(wn_copy.start)

    S.add("err there", ["here"], 0.03, err_there, sends=("next weights", "weights", 4.8, 0.0),
          gets=("at", SWAP_START + 2 * SWAP_FIELD))
    S.add("next weights", [], 0.01, lambda: pl.when(has_next)(wn_copy.wait_recv), gets="next weights")
    S.add("diagonal", [], 0.6, diagonal, gets=("at", 11.5))

    for n, k in enumerate(pieces):
        S.add(("cof", k), ["here"], 0.02, arrivals[2 + n].wait_recv,
              gets=("at", SWAP_START + SWAP_FIELD * (2 + 4.0 * (n + 1) / many)))

    def whole_rows(it, i, k):
        if it == 0:
            return []
        return [("image", it - 1, i, k)]

    def adjoint_out(it, side, i):
        row = edge_row(side)
        go[it, side, i] = c[1, i, row] * (qn if i else qb)[it, row]
        pl.when(ways[side])(edge_copy(go, gi, g_send, adjoint_sem, it, side, i).start)

    def edges_in(out, into, ssem, rsem, it, side, i):
        pl.when(ways[side])(edge_copy(out, into, ssem, rsem, it, side, i).wait_recv)

    def store_image(it, i, k):
        y[it, i, rowset(k)] = image(it, i, k)
        if i == 0 and it + 1 < ITERS:
            pl.when(has_prev)(back_copy(it + 1, k).start)

    for it in range(ITERS):
        for side, k in ((0, 0), (1, final)):
            for i in range(2):
                if it > 0:
                    needs = [("here", it - 1, k), ("adjoint in", it - 1, side, i), "diagonal"]
                    needs += [("next", it - 1, k)] if i else [("forth", it - 1, k)]
                    S.add(("edges out", it, side, i), needs, 0.06, functools.partial(edges_out, it, side, i),
                          sends=(("edges", it, side, i), ("tile", side), TILE_HOPS[side], 0.05))
                if it > 0:
                    S.add(("edges in", it, side, i), [], 0.02,
                          functools.partial(edges_in, eo, ei, h_send, edge_sem, it, side, i),
                          gets=("edges", it, side, i))
                elif i == 0:
                    S.add(("edges in", 0, side), [], 0.02, functools.partial(
                        pl.when(ways[side]), all_of(ei.at[0, side], f_recv.at[side]).wait), gets=("at", 7.7))
                S.add(("adjoint out", it, side, i), [("next" if i else "here", it, k)], 0.03,
                      functools.partial(adjoint_out, it, side, i),
                      sends=(("adjoint", it, side, i), ("tile", side), TILE_HOPS[side], 0.05))
                S.add(("adjoint in", it, side, i), [], 0.02,
                      functools.partial(edges_in, go, gi, g_send, adjoint_sem, it, side, i),
                      gets=("adjoint", it, side, i))
        for k in range(blocks):
            if it > 0:
                S.add(("back", it, k), [], 0.02, lambda it=it, k=k: pl.when(has_next)(
                    back_copy(it, k).wait_recv), gets=("back", it, k))
            elif k == 0:
                S.add(("back", 0), [], 0.02, functools.partial(
                    pl.when(has_next), all_of(vn.at[0], f_recv.at[2]).wait), gets=("at", 10.2))
            S.add(("forth", it, k), [], 0.02, lambda it=it, k=k: pl.when(has_prev)(
                forth_copy(it, k).wait_recv), gets=("forth", it, k))
            around = [m for m in (k - 1, k, k + 1) if 0 <= m < blocks]
            ends = [side for side, m in ((0, 0), (1, final)) if m == k]
            for i in range(2):
                needs = [("cof", k)] + [("edges in", it, side) + ((i,) if it else ()) for side in ends]
                for m in around:
                    needs += whole_rows(it, i, m)
                S.add(("model", it, i, k), needs, 0.05, functools.partial(model, it, i, k),
                      sends=(("forth", it, k), "forth", HOP, BLOCK) if i == 1 else None)
                needs = ["diagonal", "here", "err there"] + [("adjoint in", it, side, i) for side in ends]
                needs += [("next" if i else "here", it, m) for m in around]
                needs += [("here", it, k)] if i else [("forth", it, k)]
                S.add(("image", it, i, k), needs, 0.06, functools.partial(store_image, it, i, k),
                      sends=(("back", it + 1, k), "back", HOP, BLOCK) if i == 0 and it + 1 < ITERS else None)
            S.add(("here", it, k), ["here", "err there", ("model", it, 0, k)] + whole_rows(it, 1, k), 0.03,
                  functools.partial(misfit_here, it, k))
            S.add(("next", it, k), ["next weights", ("model", it, 1, k), ("back", it) + ((k,) if it else ())], 0.03,
                  functools.partial(misfit_next, it, k))
            S.add(("ret out", it, k), [("image", it, 0, k), ("image", it, 1, k)], 0.02,
                  lambda it=it, k=k: ret_copy(it, k).start(),
                  sends=(("ret", it, k), "ret", HOP, BLOCK))
            if it == ITERS - 1:
                S.add(("ret", it, k), [], 0.01, ret_copy(it, k).wait_recv, gets=("ret", it, k))

    S.add("ret", ["early in"], 0.01, all_of(rt.at[pl.ds(0, ITERS - 1)], rt_recv.at[blocks]).wait)

    def images(it):
        return [("image", it, i, k) for i in range(2) for k in range(blocks)]

    def moment(n, a, b):
        early[n:n + 1] = lanes(a, b)

    S.add("moment 0", [], 0.15, lambda: moment(0, v, v))
    S.add("moment 1", images(0), 0.3, lambda: (moment(1, v, y.at[0]), moment(2, y.at[0], y.at[0])))
    S.add("moment 3", images(1), 0.3,
          lambda: (moment(3, y.at[0], y.at[1]), moment(4, y.at[1], y.at[1])))

    S.add("early out", ["moment 0", "moment 1", "moment 3", *[("model", 2, 1, k) for k in range(blocks)]] + met_all, 0.4,
          lambda: to_all(early, reds, 0), sends=("early", "all", REDUCE, 0.0))

    def energy_states():
        total = None
        first = jnp.where(has_prev, 0.0, 1.0)
        for k in range(blocks):
            at = slice(k * EDGE, (k + 1) * EDGE)
            a, b = states[2][0, at], states[2][1, at]
            here = (d[0, at] + first * w[0, at]) * (a * a) + d[1, at] * (b * b)
            total = here if total is None else total + here
        energy[...] = total

    def energy_misfits(k):
        at = rowset(k)
        energy[...] += (qb[2, at] * (states[2][1, at] - u[2, 0, at])
                        + qn[2, at] * (vn[2, at] - u[2, 1, at]))

    def late_out():
        late[...] = folded(energy[...])
        to_all(late, lasts, 1)

    S.add("energy", images(1), 0.1, energy_states)
    for k in range(blocks):
        S.add(("energy", k), ["energy", ("here", 2, k), ("next", 2, k)], 0.04,
              functools.partial(energy_misfits, k))
    S.add("late out", [("energy", k) for k in range(blocks)] + met_all, 0.5, late_out,
          sends=("late", "all", REDUCE, 0.0))

    def early_in():
        m = from_all(reds, 0)
        plain = jnp.sum(m[0], axis=1, keepdims=True)
        g0 = plain[0:1]
        a0 = g0 / plain[1:2]
        less = pair_add(pair_rows(m, 0, 4), pair_scale(pair_rows(m, 1, 5), -a0))
        less = pair_add(pair_rows(less, 0, 3), pair_scale(pair_rows(less, 1, 4), -a0))
        one = pair_total(less)
        g1, d1 = one[0:1], one[1:2]
        b1 = g1 / g0
        a1 = g1 / (d1 - b1 * g1 / a0)
        p1 = -(a0 + a1 + a1 * b1)
        p2 = a0 * a1
        q = pair_add(pair_add(pair_rows(m, 0, 3), pair_scale(pair_rows(m, 1, 4), p1)),
                     pair_scale(pair_rows(m, 2, 5), p2))
        g2 = pair_total(pair_add(pair_add(pair_rows(q, 0, 1), pair_scale(pair_rows(q, 1, 2), p1)),
                                 pair_scale(pair_rows(q, 2, 3), p2)))
        rest = pair_add(pair_rows(m, 3, 4), pair_scale(pair_rows(m, 4, 5), p1))
        base = pair_add(pair_add(pair_rows(q, 1, 2), pair_scale(pair_rows(q, 2, 3), p1)),
                        pair_scale(rest, p2))
        scalars.update(a0=a0, a1=a1, b1=b1, p1=p1, p2=p2, g2=g2, b2=g2 / g1, base=base)

    S.add("early in", ["late out"], 0.6, early_in, gets="early")

    def late_in():
        s = scalars
        m = from_all(lasts, 1)
        d2 = pair_total(pair_add(s["base"], pair_scale(pair_scale(m, s["p2"]), s["p2"])))
        scalars["a2"] = s["g2"] / (d2 - s["b2"] * s["g2"] / s["a1"])

    S.add("late in", ["early in", "sent"], 0.4, late_in, gets="late")

    def own(level):
        return lambda at: v[level, at], lambda it, at: y[it, level, at]

    def away():
        return lambda at: home[at], lambda it, at: rt[it, at]

    def solve(level, source, k):
        s = scalars
        at = rowset(k)
        first, images_of = source
        r0, y0, y1 = first(at), images_of(0, at), images_of(1, at)
        p = (r0 - s["a0"] * y0) + s["b1"] * r0
        r2 = (r0 + s["p1"] * y0) + s["p2"] * y1
        x_out[0, level, at] = s["a0"] * r0 + s["a1"] * p
        r_out[0, level, at] = r2
        step[level, at] = r2 + s["b2"] * p

    def tail(level, source, k):
        s = scalars
        at = rowset(k)
        _, images_of = source
        y0, y1, y2 = images_of(0, at), images_of(1, at), images_of(2, at)
        s1 = (y0 - s["a0"] * y1) + s["b1"] * y0
        grad[level, at] = ((y0 + s["p1"] * y1) + s["p2"] * y2) + s["b2"] * s1

    def finish(level, k):
        at = rowset(k)
        x_out[0, level, at] = x_out[0, level, at] + scalars["a2"] * step[level, at]
        r_out[0, level, at] = r_out[0, level, at] - scalars["a2"] * grad[level, at]

    for k in range(blocks):
        S.add(("solve own", k), ["early in"] + [("image", it, i, k) for it in range(2) for i in range(2)],
              0.06, functools.partial(solve, lev, own(lev), k))
        S.add(("solve away", k), ["early in", "here", "ret"],
              0.06, functools.partial(solve, other, away(), k))
        S.add(("tail own", k), ["early in"] + [("image", it, i, k) for it in range(3) for i in range(2)],
              0.06, functools.partial(tail, lev, own(lev), k))
        S.add(("tail away", k), ["early in", "ret", ("ret", ITERS - 1, k)],
              0.06, functools.partial(tail, other, away(), k))
        S.add(("finish own", k), ["late in", ("solve own", k), ("tail own", k)],
              0.04, functools.partial(finish, lev, k))
        S.add(("finish away", k), ["late in", ("solve away", k), ("tail away", k)],
              0.04, functools.partial(finish, other, k))

    def sent():
        all_of(y, xs_sem.at[0]).wait()
        ob_copy.wait_send()
        pl.when(has_prev)(wn_copy.wait_send)
        for side in range(2):
            pl.when(ways[side])(all_of(eo.at[:, side], h_send.at[side]).wait)
            pl.when(ways[side])(all_of(go.at[:, side], g_send.at[side]).wait)
        all_of(rt, rt_send).wait()
        pl.when(has_prev)(all_of(vn, b_send.at[0]).wait)
        pl.when(has_next)(all_of(ui, b_send.at[1]).wait)
        all_of(reds.at[pl.ds(0, count - 1)], rd_send.at[0]).wait()

    S.add("sent", [("tail away", k) for k in range(blocks)], 0.5, sent)
    order = S.order()
    if SHOW:
        for name, _, when in order:
            print(f"{when:6.2f}", name)
    for name, run, _ in order:
        run()

    most = lasts.at[pl.ds(0, count - 1)]
    pltpu.make_async_copy(most, most, rd_send.at[1]).wait()


SHOW = False


def on_device(wins, tiles, right_side, error_weight, coeffs, obs_block, obs_pos, obs_weight):
    _, levels, rows, cols = right_side.shape
    nblk, width = obs_pos.shape[1:]
    f32 = jnp.float32
    vm = functools.partial(pltpu.VMEM, dtype=f32)
    dma = pltpu.SemaphoreType.DMA
    hbm = pl.BlockSpec(memory_space=pltpu.HBM)
    vmem = pl.BlockSpec(memory_space=pltpu.VMEM)
    blocks = rows // EDGE
    field = (rows, cols)
    edge = vm((ITERS, 2, 2, 1, cols))
    scratch = [
        pltpu.VMEM(obs_block.shape, jnp.int32),
        pltpu.VMEM(obs_pos.shape, jnp.int32),
        vm(obs_weight.shape),
        vm((2,) + field),
        vm((ITERS, 2) + field),
        vm((2,) + field),
        vm(field),
        vm((4, 2) + field),
        vm((2,) + field),
        vm((2, nblk + 8, width)),
        vm((ITERS, 2) + field),
        vm((ITERS,) + field),
        vm((ITERS,) + field),
        vm((ITERS,) + field),
        vm((ITERS,) + field),
        edge, edge, edge, edge,
        vm((ITERS,) + field),
        vm(field),
        vm((2,) + field),
        vm((2,) + field),
        vm((EDGE, cols)),
        vm((MOMENTS, width)),
        vm((1, width)),
        vm((wins * tiles, MOMENTS, width)),
        vm((wins * tiles, 1, width)),
        dma((3 + blocks,)), dma((2,)), dma((5,)),
        dma((3,)), dma((2,)), dma((ITERS - 1, 2, 2)),
        dma((2,)), dma((ITERS - 1, blocks)), dma((ITERS, blocks)),
        dma((2,)), dma((ITERS, 2, 2)),
        dma, dma((1 + blocks,)),
        dma((2,)), dma((2,)),
        dma, dma,
        pltpu.SemaphoreType.REGULAR((1 + len(doubling(tiles)) + len(doubling(wins // 2)),)),
    ]
    out = vm(right_side.shape)
    return pl.pallas_call(
        functools.partial(kernel, wins, tiles),
        out_shape=(out, out),
        in_specs=[hbm] * 6,
        out_specs=(vmem, vmem),
        scratch_shapes=scratch,
        compiler_params=pltpu.CompilerParams(has_side_effects=True, collective_id=0,
                                             vmem_limit_bytes=60 * 1024 * 1024),
    )(right_side, error_weight, coeffs, obs_block, obs_pos, obs_weight)


def solution(mesh):
    in_specs = (
        P("win", None, "tile", None),
        P("win", None, "tile", None),
        P(None, "win", None, "tile", None),
        P("win", "tile"),
        P("win", "tile", None),
        P("win", "tile", None),
    )
    out_specs = (P("win", None, "tile", None), P("win", None, "tile", None))
    return jax.shard_map(
        functools.partial(on_device, mesh.shape["win"], mesh.shape["tile"]),
        mesh=mesh, in_specs=in_specs, out_specs=out_specs, check_vma=False
    )
```

```python
import functools

import jax
import jax.numpy as jnp
from jax import lax
from jax.experimental import pallas as pl
from jax.experimental.pallas import tpu as pltpu
from jax.sharding import PartitionSpec as P

ITERS = 3
EDGE = 8
MOMENTS = 2 * ITERS - 1

HOP, TILE_HOPS, BLOCK, SWAP_START, SWAP_FIELD, REDUCE, BEGIN = 2.40, (3.30, 1.50), 0.70, 2.20, 2.83, 5.31, 7.50


def doubling(length):
    steps, known = [], 1
    while known < length - 1:
        steps.append(known)
        known *= 2
    return steps


HINTS = {('back', 2): -1.4, 'early out': 1.3, ('model', 1): -0.87}
STEP = 1.00


class Steps:
    def __init__(self):
        self.todo = {}

    def add(self, name, needs, cost, run, sends=None, gets=None):
        self.todo[name] = (list(needs), cost, run, sends, gets)

    def order(self):
        senders = {sends[0]: name for name, (_, _, _, sends, _) in self.todo.items() if sends}
        after = {name: [] for name in self.todo}
        for name, (needs, _, _, _, gets) in self.todo.items():
            for need in needs:
                after[need].append((name, 0.0))
            if gets in senders:
                after[senders[gets]].append((name, self.todo[senders[gets]][3][2]))
        rank = {}

        def path(name):
            if name not in rank:
                rank[name] = self.todo[name][1] + max(
                    (wait + path(then) for then, wait in after[name]), default=0.0)
            return rank[name]

        for name in self.todo:
            path(name)
        for name in self.todo:
            kind = name if isinstance(name, str) else name[:2]
            rank[name] += HINTS.get(kind, 0.0)
        now, done, arrive, free, result = BEGIN, set(), {}, {}, []
        for _, (_, _, _, _, gets) in self.todo.items():
            if isinstance(gets, tuple) and gets[0] == "at":
                arrive[gets] = gets[1]
        left = dict(self.todo)
        while left:
            ready, soon = None, None
            for name, (needs, _, _, _, gets) in left.items():
                if any(need not in done for need in needs):
                    continue
                at = arrive.get(gets, None) if gets is not None else 0.0
                if at is None:
                    continue
                if at <= now:
                    if ready is None or rank[name] > rank[ready]:
                        ready = name
                elif soon is None or at < soon[0]:
                    soon = (at, name)
            pick = ready
            if pick is None:
                now, pick = soon
            _, cost, run, sends, _ = left.pop(pick)
            now += STEP * cost
            done.add(pick)
            if sends:
                message, link, latency, busy = sends
                begin = max(now, free.get(link, 0.0))
                free[link] = begin + busy
                arrive[message] = begin + busy + latency
            result.append((pick, run, now))
        return result


def two_sum(a, b):
    total = a + b
    back = total - a
    return total, (a - (total - back)) + (b - back)


def halves(a):
    big = 4097.0 * a
    high = big - (big - a)
    return high, a - high


def two_product(a, b):
    (ah, al), (bh, bl) = halves(a), halves(b)
    product = a * b
    return product, ((ah * bh - product) + ah * bl + al * bh) + al * bl


def pair_add(a, b):
    total, rest = two_sum(a[0], b[0])
    rest = rest + (a[1] + b[1])
    high = total + rest
    return high, rest - (high - total)


def pair_scale(a, factor):
    product, rest = two_product(a[0], factor)
    rest = rest + a[1] * factor
    high = product + rest
    return high, rest - (high - product)


def pair_rows(a, lo, hi):
    return a[0][lo:hi], a[1][lo:hi]


def pair_total(a):
    return jnp.sum(a[0], axis=1, keepdims=True) + jnp.sum(a[1], axis=1, keepdims=True)


def kernel(wins, tiles, rhs, err, cof, oblk_in, opos_in, owgt_in, x_out, r_out,
           obk, ops, owt, v, y, w, wn, c, d, ob, u, ui, vn, qb, qn, eo, ei, go, gi, rt, home, far, ahead,
           step, grad, energy, early, late, reds, lasts,
           x_sem, xs_sem, l_sem, f_recv, h_send, h_recv, b_send, b_recv, c_recv, g_send, g_recv,
           rt_send, rt_recv, rd_send, rd_recv, wn_send, wn_recv, hello):
    me_w = lax.axis_index("win")
    me_t = lax.axis_index("tile")
    lev = lax.rem(me_w, 2)
    other = 1 - lev
    mate = me_w + 1 - 2 * lev
    has_next = me_w + 2 < wins
    has_prev = me_w >= 2
    rows, cols = v.shape[1], v.shape[2]
    count = wins * tiles
    me = me_w * tiles + me_t
    width = ops.shape[2]
    nblk = ops.shape[1]
    last = rows - 1
    blocks = rows // EDGE
    final = blocks - 1
    pieces = list(range(final - 1)) + [final, final - 1]
    many = len(pieces)
    f32 = jnp.float32

    odd = lax.rem(me_t, 2)
    even = odd == 0

    def first_row(k):
        return pl.multiple_of((k + odd * (final - 2 * k)) * EDGE, EDGE)

    def rowset(k):
        return pl.ds(first_row(k), EDGE)

    def row_beyond(k, side):
        return pl.ds(first_row(k) - 1 + 9 * odd if side == 0 else first_row(k) + EDGE - 9 * odd, 1)

    def edge_row(side):
        return pl.ds(odd * last if side == 0 else last - odd * last, 1)

    beside = (me_t - 1 + 2 * odd, me_t + 1 - 2 * odd)
    ways = tuple(jnp.logical_and(tile >= 0, tile < tiles) for tile in beside)

    def remote(src, dst, ssem, rsem, win, tile):
        return pltpu.make_async_remote_copy(
            src_ref=src, dst_ref=dst, send_sem=ssem, recv_sem=rsem,
            device_id=(win, tile), device_id_type=pl.DeviceIdType.MESH)

    def all_of(ref, sem):
        return pltpu.make_async_copy(ref, ref, sem)

    barrier = pltpu.get_barrier_semaphore()

    def signal(sem, win, tile):
        pl.semaphore_signal(sem, inc=1, device_id=(win, tile), device_id_type=pl.DeviceIdType.MESH)

    def greet(sem, ends):
        for there, win, tile in ends:
            pl.when(there)(functools.partial(signal, sem, win, tile))

    def met(sem, ends):
        pl.semaphore_wait(sem, sum(there.astype(jnp.int32) for there, _, _ in ends))

    def along_tile(hop):
        return [(me_t >= hop, me_w, me_t - hop), (me_t + hop < tiles, me_w, me_t + hop)]

    def along_win(hop):
        return [(me_w >= 2 * hop, me_w - 2 * hop, me_t),
                (me_w + 2 * hop < wins, me_w + 2 * hop, me_t)]

    facing = [(me_w >= 0, mate, me_t)]
    near = facing + along_tile(1) + along_win(1)
    rounds = ([along_tile(hop) for hop in doubling(tiles)] + [facing]
              + [along_win(hop) for hop in doubling(wins // 2)])

    greet(barrier, near)

    swaps = [
        remote(rhs.at[0, other], v.at[lev], xs_sem.at[0], x_sem.at[0], mate, me_t),
        remote(err.at[0, other], w.at[lev], xs_sem.at[0], x_sem.at[1], mate, me_t),
    ] + [
        remote(cof.at[:, 0, other, rowset(k)], c.at[:, lev, rowset(k)],
               xs_sem.at[0], x_sem.at[3 + n], mate, me_t)
        for n, k in enumerate(pieces)
    ]
    arrivals = [
        remote(rhs.at[0, other], v.at[other], xs_sem.at[0], x_sem.at[0], mate, me_t),
        remote(err.at[0, other], w.at[other], xs_sem.at[0], x_sem.at[1], mate, me_t),
    ] + [
        remote(cof.at[:, 0, other, rowset(k)], c.at[:, other, rowset(k)],
               xs_sem.at[0], x_sem.at[3 + n], mate, me_t)
        for n, k in enumerate(pieces)
    ]
    locs = {
        "block": pltpu.make_async_copy(oblk_in, obk, l_sem.at[0]),
        "pos": pltpu.make_async_copy(opos_in, ops, l_sem.at[1]),
        "weight": pltpu.make_async_copy(owgt_in, owt, l_sem.at[4]),
        "rhs": pltpu.make_async_copy(rhs.at[0, lev], v.at[lev], l_sem.at[2]),
        "err": pltpu.make_async_copy(err.at[0, lev], w.at[lev], l_sem.at[3]),
        "home": pltpu.make_async_copy(rhs.at[0, other], home, l_sem.at[3]),
        "cof": pltpu.make_async_copy(cof.at[:, 0, lev], c.at[:, lev], l_sem.at[3]),
        "far": pltpu.make_async_copy(cof.at[:, 0, other, rowset(pieces[-1])], far, l_sem.at[5]),
    }
    for one in locs.values():
        one.start()
    met(barrier, near)
    for one in swaps[:3]:
        one.start()
    greet(hello.at[0], rounds[0])

    for side in range(2):
        @pl.when(jnp.logical_not(ways[side]))
        def _():
            for it in range(ITERS):
                ei[it, side] = jnp.zeros(ei.shape[2:], f32)
                gi[it, side] = jnp.zeros(gi.shape[2:], f32)

    @pl.when(jnp.logical_not(has_prev))
    def _():
        for it in range(ITERS):
            ui[it] = jnp.zeros(ui.shape[1:], f32)

    @pl.when(jnp.logical_not(has_next))
    def _():
        wn[...] = jnp.zeros(wn.shape, f32)
        for it in range(ITERS):
            vn[it] = jnp.zeros(vn.shape[1:], f32)

    states = (v, y.at[0], y.at[1])
    row8 = lax.broadcasted_iota(jnp.int32, (EDGE, cols), 0)

    def east(a):
        return pltpu.roll(a, cols - 1, 1)

    def west(a):
        return pltpu.roll(a, 1, 1)

    def sides(a, beyond):
        top, bottom = jnp.where(even, beyond[0], beyond[1]), jnp.where(even, beyond[1], beyond[0])
        return (jnp.where(row8 == 0, top, pltpu.roll(a, 1, 0))
                + jnp.where(row8 == EDGE - 1, bottom, pltpu.roll(a, EDGE - 1, 0)))

    def edge_copy(out, into, ssem, rsem, it, side, i):
        return remote(out.at[it, side, i], into.at[it, side, i], ssem.at[side],
                      rsem(it, side, i), me_w, beside[side])

    def edge_sem(it, side, i):
        return f_recv.at[side] if it == 0 else h_recv.at[it - 1, side, i]

    def adjoint_sem(it, side, i):
        return g_recv.at[it, side, i]


    def back_copy(it, k):
        return remote(states[it].at[0, rowset(k)], vn.at[it, rowset(k)],
                      b_send.at[0], b_recv.at[it - 1, k] if it else f_recv.at[2], me_w - 2, me_t)

    def forth_copy(it, k):
        return remote(u.at[it, 1, rowset(k)], ui.at[it, rowset(k)],
                      b_send.at[2 if it else 1], c_recv.at[it, k], me_w + 2, me_t)

    def ret_copy(it, k):
        return remote(y.at[it, other, rowset(k)], rt.at[it, rowset(k)],
                      rt_send, rt_recv.at[k if it == ITERS - 1 else blocks], mate, me_t)

    sends_ahead = jnp.logical_and(lev == 1, has_next)

    def ahead_copy(n):
        return remote(ahead.at[n], ui.at[0, rowset(pieces[-1])], b_send.at[3],
                      c_recv.at[0, pieces[-1]], me_w + 2 - n, me_t)

    wn_copy = remote(w.at[0], wn, wn_send, wn_recv, me_w - 2, me_t)

    def end_side(k):
        return 0 if k == 0 else 1 if k == final else None

    def model(it, i, k):
        src, at = states[it], rowset(k)
        a = src[i, at]
        beyond = [ei[it, side, i] if side == end_side(k) else src[i, row_beyond(k, side)]
                  for side in range(2)]
        u[it, i, at] = (c[0, i, at] * a + c[1, i, at] * sides(a, beyond)
                        + c[2, i, at] * east(a) + c[3, i, at] * west(a))
        if i == 1 and (it, k) != (0, pieces[-1]):
            pl.when(has_next)(forth_copy(it, k).start)

    def misfit_here(it, k):
        at = rowset(k)
        qb[it, at] = w[1, at] * (states[it][1, at] - u[it, 0, at])

    def misfit_next(it, k):
        at = rowset(k)
        qn[it, at] = wn[at] * (vn[it, at] - u[it, 1, at])

    def adjoint(it, i, q, k, alone=None):
        at = rowset(k)
        a = q[it, at]
        beyond = []
        for side in range(2):
            if side == end_side(k):
                beyond.append(gi[it, side, i])
            elif alone is not None:
                beyond.append(jnp.zeros((1, cols), f32))
            else:
                row = row_beyond(k, side)
                beyond.append(c[1, i, row] * q[it, row])
        return (c[0, i, at] * a + sides(c[1, i, at] * a, beyond)
                + west(c[2, i, at] * a) + east(c[3, i, at] * a))

    def image(it, i, k, alone=None):
        at = rowset(k)
        src = states[it]
        if i == 1:
            return (qb[it, at] + d[1, at] * src[1, at]) - adjoint(it, 1, qn, k, alone)
        return (d[0, at] * src[0, at] - adjoint(it, 0, qb, k, alone)) + w[0, at] * (src[0, at] - ui[it, at])

    def diagonal():
        ob_back.wait_recv()
        per_row = cols // width
        base = lev * (rows * per_row)
        spot = lax.broadcasted_iota(jnp.int32, (rows, nblk), 0) * per_row + base
        for i in range(2):
            who = ob[i, nblk:nblk + 1, 0:nblk]
            sums = ob[i, 0:nblk, :]
            for k in range(per_row):
                hot = jnp.where((spot + k).astype(f32) == who, 1.0, 0.0)
                d[i, :, k * width:(k + 1) * width] = jnp.dot(
                    hot, sums, precision=lax.Precision.HIGHEST, preferred_element_type=f32)

    def lanes(a, b):
        total = None
        for k in range(blocks):
            at = slice(k * EDGE, (k + 1) * EDGE)
            here = a[0, at] * b[0, at] + a[1, at] * b[1, at]
            total = here if total is None else total + here
        return folded(total)

    def folded(total):
        total = jnp.sum(total, axis=0, keepdims=True)
        parts = [total[:, k * width:(k + 1) * width] for k in range(cols // width)]
        while len(parts) > 1:
            parts = [sum(parts[k:k + 2]) for k in range(0, len(parts), 2)]
        return parts[0]

    def to_all(part, into, sems):
        turned = 2 * me < count

        def send(o, carry):
            to = lax.rem(me + jnp.where(turned, count - o, o), count)
            remote(part, into.at[me], rd_send.at[sems], rd_recv.at[sems],
                   to // tiles, lax.rem(to, tiles)).start()
            return carry

        lax.fori_loop(1, count, send, 0)
        into[me] = part[...]

    def from_all(into, sems):
        most = into.at[pl.ds(0, count - 1)]
        pltpu.make_async_copy(most, most, rd_recv.at[sems]).wait()
        high, low = into[0], jnp.zeros(into.shape[1:], f32)
        for k in range(1, count):
            high, rest = two_sum(high, into[k])
            low = low + rest
        return high, low

    def edges_out(it, side, i):
        if it == 0:
            eo[it, side, i] = v[i, edge_row(side)]
        else:
            whole = image(it - 1, i, 0 if side == 0 else final, alone=True)
            low, high = whole[0:1], whole[EDGE - 1:EDGE]
            eo[it, side, i] = jnp.where(even, low, high) if side == 0 else jnp.where(even, high, low)
        pl.when(ways[side])(edge_copy(eo, ei, h_send, edge_sem, it, side, i).start)

    for one in ("block", "pos", "weight"):
        locs[one].wait()
    cell = lax.broadcasted_iota(jnp.int32, (width, width), 0)
    ones = jnp.ones((8, width), f32)
    ob[lev, nblk:, :] = jnp.zeros((8, width), f32)

    def per_block(b, carry):
        hit = jnp.where(cell == ops[0, pl.ds(b, 1), :], owt[0, pl.ds(b, 1), :], 0.0)
        total = lax.dot_general(ones, hit, (((1,), (1,)), ((), ())),
                                precision=lax.Precision.HIGHEST,
                                preferred_element_type=f32)
        ob[lev, pl.ds(b, 1), :] = total[0:1]
        return carry

    most = nblk - nblk // 4
    lax.fori_loop(0, most, per_block, 0)
    locs["rhs"].wait()
    arrivals[0].wait_recv()
    swaps[3].start()
    for k in range(blocks):
        pl.when(has_prev)(back_copy(0, k).start)
    for side in range(2):
        for i in range(2):
            edges_out(0, side, i)
    all_of(y, l_sem.at[3]).wait()
    locs["far"].wait()

    @pl.when(sends_ahead)
    def _():
        at = rowset(pieces[-1])
        rims = [row_beyond(pieces[-1], side) for side in range(2)]
        for n, (a, beyond, k) in enumerate((
                (v[lev, at], [v[lev, row] for row in rims], [c[m, lev, at] for m in range(4)]),
                (home[at], [home[row] for row in rims], [far[m] for m in range(4)]))):
            ahead[n] = k[0] * a + k[1] * sides(a, beyond) + k[2] * east(a) + k[3] * west(a)
            ahead_copy(n).start()

    lax.fori_loop(most, nblk, per_block, 0)
    ob[lev, nblk:nblk + 1, 0:nblk] = obk[...].astype(f32)
    ob_copy = remote(ob.at[lev], ob.at[lev], xs_sem.at[1], x_sem.at[2], mate, me_t)
    ob_back = remote(ob.at[lev], ob.at[other], xs_sem.at[1], x_sem.at[2], mate, me_t)
    ob_copy.start()
    for one in swaps[4:]:
        one.start()

    S = Steps()
    scalars = {}

    def spread(at):
        met(hello.at[at], rounds[at])
        if at + 1 < len(rounds):
            greet(hello.at[at + 1], rounds[at + 1])

    for n in range(len(rounds)):
        S.add(("spread", n), [("spread", n - 1)] if n else [], 0.05, functools.partial(spread, n),
              sends=(("hello", n), "hello", 3.0, 0.0), gets=("hello", n - 1) if n else ("at", 1.5))
    met_all = [("spread", len(rounds) - 1)]

    S.add("here", [], 0.0, lambda: None)

    def err_there():
        arrivals[1].wait_recv()
        pl.when(has_prev)(wn_copy.start)

    S.add("err there", ["here"], 0.03, err_there, sends=("next weights", "weights", 4.8, 0.0),
          gets=("at", SWAP_START + 2 * SWAP_FIELD))
    S.add("next weights", [], 0.01, lambda: pl.when(has_next)(wn_copy.wait_recv), gets="next weights")
    S.add("diagonal", [], 0.6, diagonal, gets=("at", 15.2))

    for n, k in enumerate(pieces):
        S.add(("cof", k), ["here"], 0.02, arrivals[2 + n].wait_recv,
              gets=("at", SWAP_START + SWAP_FIELD * (2 + 4.0 * (n + 1) / many)))

    def whole_rows(it, i, k):
        if it == 0:
            return []
        return [("image", it - 1, i, k)]

    def adjoint_out(it, side, i):
        row = edge_row(side)
        go[it, side, i] = c[1, i, row] * (qn if i else qb)[it, row]
        pl.when(ways[side])(edge_copy(go, gi, g_send, adjoint_sem, it, side, i).start)

    def edges_in(out, into, ssem, rsem, it, side, i):
        pl.when(ways[side])(edge_copy(out, into, ssem, rsem, it, side, i).wait_recv)

    def store_image(it, i, k):
        y[it, i, rowset(k)] = image(it, i, k)
        if i == 0 and it + 1 < ITERS:
            pl.when(has_prev)(back_copy(it + 1, k).start)

    for it in range(ITERS):
        for side, k in ((0, 0), (1, final)):
            for i in range(2):
                if it > 0:
                    needs = [("here", it - 1, k), ("adjoint in", it - 1, side, i), "diagonal"]
                    needs += [("next", it - 1, k)] if i else [("forth", it - 1, k)]
                    S.add(("edges out", it, side, i), needs, 0.06, functools.partial(edges_out, it, side, i),
                          sends=(("edges", it, side, i), ("tile", side), TILE_HOPS[side], 0.05))
                if it > 0:
                    S.add(("edges in", it, side, i), [], 0.02,
                          functools.partial(edges_in, eo, ei, h_send, edge_sem, it, side, i),
                          gets=("edges", it, side, i))
                elif i == 0:
                    S.add(("edges in", 0, side), [], 0.02, functools.partial(
                        pl.when(ways[side]), all_of(ei.at[0, side], f_recv.at[side]).wait), gets=("at", 7.7))
                S.add(("adjoint out", it, side, i), [("next" if i else "here", it, k)], 0.03,
                      functools.partial(adjoint_out, it, side, i),
                      sends=(("adjoint", it, side, i), ("tile", side), TILE_HOPS[side], 0.05))
                S.add(("adjoint in", it, side, i), [], 0.02,
                      functools.partial(edges_in, go, gi, g_send, adjoint_sem, it, side, i),
                      gets=("adjoint", it, side, i))
        for k in range(blocks):
            if it > 0:
                S.add(("back", it, k), [], 0.02, lambda it=it, k=k: pl.when(has_next)(
                    back_copy(it, k).wait_recv), gets=("back", it, k))
            elif k == 0:
                S.add(("back", 0), [], 0.02, functools.partial(
                    pl.when(has_next), all_of(vn.at[0], f_recv.at[2]).wait), gets=("at", 10.2))
            S.add(("forth", it, k), [], 0.02, lambda it=it, k=k: pl.when(has_prev)(
                forth_copy(it, k).wait_recv),
                  gets=("at", 10.5) if (it, k) == (0, pieces[-1]) else ("forth", it, k))
            around = [m for m in (k - 1, k, k + 1) if 0 <= m < blocks]
            ends = [side for side, m in ((0, 0), (1, final)) if m == k]
            for i in range(2):
                needs = [("cof", k)] + [("edges in", it, side) + ((i,) if it else ()) for side in ends]
                for m in around:
                    needs += whole_rows(it, i, m)
                S.add(("model", it, i, k), needs, 0.05, functools.partial(model, it, i, k),
                      sends=(("forth", it, k), "forth", HOP, BLOCK)
                      if i == 1 and (it, k) != (0, pieces[-1]) else None)
                needs = ["diagonal", "here", "err there"] + [("adjoint in", it, side, i) for side in ends]
                needs += [("next" if i else "here", it, m) for m in around]
                needs += [("here", it, k)] if i else [("forth", it, k)]
                S.add(("image", it, i, k), needs, 0.06, functools.partial(store_image, it, i, k),
                      sends=(("back", it + 1, k), "back", HOP, BLOCK) if i == 0 and it + 1 < ITERS else None)
            S.add(("here", it, k), ["here", "err there", ("model", it, 0, k)] + whole_rows(it, 1, k), 0.03,
                  functools.partial(misfit_here, it, k))
            S.add(("next", it, k), ["next weights", ("model", it, 1, k), ("back", it) + ((k,) if it else ())], 0.03,
                  functools.partial(misfit_next, it, k))
            S.add(("ret out", it, k), [("image", it, 0, k), ("image", it, 1, k)], 0.02,
                  lambda it=it, k=k: ret_copy(it, k).start(),
                  sends=(("ret", it, k), "ret", HOP, BLOCK))
            if it == ITERS - 1:
                S.add(("ret", it, k), [], 0.01, ret_copy(it, k).wait_recv, gets=("ret", it, k))

    S.add("ret", ["early in"], 0.01, all_of(rt.at[pl.ds(0, ITERS - 1)], rt_recv.at[blocks]).wait)

    def images(it):
        return [("image", it, i, k) for i in range(2) for k in range(blocks)]

    def moment(n, a, b):
        early[n:n + 1] = lanes(a, b)

    S.add("moment 0", [], 0.15, lambda: moment(0, v, v))
    S.add("moment 1", images(0), 0.3, lambda: (moment(1, v, y.at[0]), moment(2, y.at[0], y.at[0])))
    S.add("moment 3", images(1), 0.3,
          lambda: (moment(3, y.at[0], y.at[1]), moment(4, y.at[1], y.at[1])))

    S.add("early out", ["moment 0", "moment 1", "moment 3", *[("model", 2, 1, k) for k in range(blocks)]] + met_all, 0.4,
          lambda: to_all(early, reds, 0), sends=("early", "all", REDUCE, 0.0))

    def energy_states():
        total = None
        first = jnp.where(has_prev, 0.0, 1.0)
        for k in range(blocks):
            at = slice(k * EDGE, (k + 1) * EDGE)
            a, b = states[2][0, at], states[2][1, at]
            here = (d[0, at] + first * w[0, at]) * (a * a) + d[1, at] * (b * b)
            total = here if total is None else total + here
        energy[...] = total

    def energy_misfits(k):
        at = rowset(k)
        energy[...] += (qb[2, at] * (states[2][1, at] - u[2, 0, at])
                        + qn[2, at] * (vn[2, at] - u[2, 1, at]))

    def late_out():
        late[...] = folded(energy[...])
        to_all(late, lasts, 1)

    S.add("energy", images(1), 0.1, energy_states)
    for k in range(blocks):
        S.add(("energy", k), ["energy", ("here", 2, k), ("next", 2, k)], 0.04,
              functools.partial(energy_misfits, k))
    S.add("late out", [("energy", k) for k in range(blocks)] + met_all, 0.5, late_out,
          sends=("late", "all", REDUCE, 0.0))

    def early_in():
        m = from_all(reds, 0)
        plain = jnp.sum(m[0], axis=1, keepdims=True)
        g0 = plain[0:1]
        a0 = g0 / plain[1:2]
        less = pair_add(pair_rows(m, 0, 4), pair_scale(pair_rows(m, 1, 5), -a0))
        less = pair_add(pair_rows(less, 0, 3), pair_scale(pair_rows(less, 1, 4), -a0))
        one = pair_total(less)
        g1, d1 = one[0:1], one[1:2]
        b1 = g1 / g0
        a1 = g1 / (d1 - b1 * g1 / a0)
        p1 = -(a0 + a1 + a1 * b1)
        p2 = a0 * a1
        q = pair_add(pair_add(pair_rows(m, 0, 3), pair_scale(pair_rows(m, 1, 4), p1)),
                     pair_scale(pair_rows(m, 2, 5), p2))
        g2 = pair_total(pair_add(pair_add(pair_rows(q, 0, 1), pair_scale(pair_rows(q, 1, 2), p1)),
                                 pair_scale(pair_rows(q, 2, 3), p2)))
        rest = pair_add(pair_rows(m, 3, 4), pair_scale(pair_rows(m, 4, 5), p1))
        base = pair_add(pair_add(pair_rows(q, 1, 2), pair_scale(pair_rows(q, 2, 3), p1)),
                        pair_scale(rest, p2))
        scalars.update(a0=a0, a1=a1, b1=b1, p1=p1, p2=p2, g2=g2, b2=g2 / g1, base=base)

    S.add("early in", ["late out"], 0.6, early_in, gets="early")

    def late_in():
        s = scalars
        m = from_all(lasts, 1)
        d2 = pair_total(pair_add(s["base"], pair_scale(pair_scale(m, s["p2"]), s["p2"])))
        scalars["a2"] = s["g2"] / (d2 - s["b2"] * s["g2"] / s["a1"])

    S.add("late in", ["early in", "sent"], 0.4, late_in, gets="late")

    def own(level):
        return lambda at: v[level, at], lambda it, at: y[it, level, at]

    def away():
        return lambda at: home[at], lambda it, at: rt[it, at]

    def solve(level, source, k):
        s = scalars
        at = rowset(k)
        first, images_of = source
        r0, y0, y1 = first(at), images_of(0, at), images_of(1, at)
        p = (r0 - s["a0"] * y0) + s["b1"] * r0
        r2 = (r0 + s["p1"] * y0) + s["p2"] * y1
        x_out[0, level, at] = s["a0"] * r0 + s["a1"] * p
        r_out[0, level, at] = r2
        step[level, at] = r2 + s["b2"] * p

    def tail(level, source, k):
        s = scalars
        at = rowset(k)
        _, images_of = source
        y0, y1, y2 = images_of(0, at), images_of(1, at), images_of(2, at)
        s1 = (y0 - s["a0"] * y1) + s["b1"] * y0
        grad[level, at] = ((y0 + s["p1"] * y1) + s["p2"] * y2) + s["b2"] * s1

    def finish(level, k):
        at = rowset(k)
        x_out[0, level, at] = x_out[0, level, at] + scalars["a2"] * step[level, at]
        r_out[0, level, at] = r_out[0, level, at] - scalars["a2"] * grad[level, at]

    for k in range(blocks):
        S.add(("solve own", k), ["early in"] + [("image", it, i, k) for it in range(2) for i in range(2)],
              0.06, functools.partial(solve, lev, own(lev), k))
        S.add(("solve away", k), ["early in", "here", "ret"],
              0.06, functools.partial(solve, other, away(), k))
        S.add(("tail own", k), ["early in"] + [("image", it, i, k) for it in range(3) for i in range(2)],
              0.06, functools.partial(tail, lev, own(lev), k))
        S.add(("tail away", k), ["early in", "ret", ("ret", ITERS - 1, k)],
              0.06, functools.partial(tail, other, away(), k))
        S.add(("finish own", k), ["late in", ("solve own", k), ("tail own", k)],
              0.04, functools.partial(finish, lev, k))
        S.add(("finish away", k), ["late in", ("solve away", k), ("tail away", k)],
              0.04, functools.partial(finish, other, k))

    def sent():
        all_of(y, xs_sem.at[0]).wait()
        ob_copy.wait_send()
        pl.when(has_prev)(wn_copy.wait_send)
        for side in range(2):
            pl.when(ways[side])(all_of(eo.at[:, side], h_send.at[side]).wait)
            pl.when(ways[side])(all_of(go.at[:, side], g_send.at[side]).wait)
        all_of(rt, rt_send).wait()
        pl.when(has_prev)(all_of(vn, b_send.at[0]).wait)
        pl.when(has_next)(all_of(ui.at[0, pl.ds(0, rows - EDGE)], b_send.at[1]).wait)
        pl.when(has_next)(all_of(ui.at[pl.ds(1, ITERS - 1)], b_send.at[2]).wait)
        pl.when(sends_ahead)(all_of(ahead, b_send.at[3]).wait)
        all_of(reds.at[pl.ds(0, count - 1)], rd_send.at[0]).wait()

    S.add("sent", [("tail away", k) for k in range(blocks)], 0.5, sent)
    order = S.order()
    for name, run, _ in order:
        run()

    most = lasts.at[pl.ds(0, count - 1)]
    pltpu.make_async_copy(most, most, rd_send.at[1]).wait()


def on_device(wins, tiles, right_side, error_weight, coeffs, obs_block, obs_pos, obs_weight):
    _, levels, rows, cols = right_side.shape
    nblk, width = obs_pos.shape[1:]
    f32 = jnp.float32
    vm = functools.partial(pltpu.VMEM, dtype=f32)
    dma = pltpu.SemaphoreType.DMA
    hbm = pl.BlockSpec(memory_space=pltpu.HBM)
    vmem = pl.BlockSpec(memory_space=pltpu.VMEM)
    blocks = rows // EDGE
    field = (rows, cols)
    edge = vm((ITERS, 2, 2, 1, cols))
    scratch = [
        pltpu.VMEM(obs_block.shape, jnp.int32),
        pltpu.VMEM(obs_pos.shape, jnp.int32),
        vm(obs_weight.shape),
        vm((2,) + field),
        vm((ITERS, 2) + field),
        vm((2,) + field),
        vm(field),
        vm((4, 2) + field),
        vm((2,) + field),
        vm((2, nblk + 8, width)),
        vm((ITERS, 2) + field),
        vm((ITERS,) + field),
        vm((ITERS,) + field),
        vm((ITERS,) + field),
        vm((ITERS,) + field),
        edge, edge, edge, edge,
        vm((ITERS,) + field),
        vm(field),
        vm((4, EDGE, cols)),
        vm((2, EDGE, cols)),
        vm((2,) + field),
        vm((2,) + field),
        vm((EDGE, cols)),
        vm((MOMENTS, width)),
        vm((1, width)),
        vm((wins * tiles, MOMENTS, width)),
        vm((wins * tiles, 1, width)),
        dma((3 + blocks,)), dma((2,)), dma((6,)),
        dma((3,)), dma((2,)), dma((ITERS - 1, 2, 2)),
        dma((4,)), dma((ITERS - 1, blocks)), dma((ITERS, blocks)),
        dma((2,)), dma((ITERS, 2, 2)),
        dma, dma((1 + blocks,)),
        dma((2,)), dma((2,)),
        dma, dma,
        pltpu.SemaphoreType.REGULAR((1 + len(doubling(tiles)) + len(doubling(wins // 2)),)),
    ]
    out = vm(right_side.shape)
    return pl.pallas_call(
        functools.partial(kernel, wins, tiles),
        out_shape=(out, out),
        in_specs=[hbm] * 6,
        out_specs=(vmem, vmem),
        scratch_shapes=scratch,
        compiler_params=pltpu.CompilerParams(has_side_effects=True, collective_id=0,
                                             vmem_limit_bytes=60 * 1024 * 1024),
    )(right_side, error_weight, coeffs, obs_block, obs_pos, obs_weight)


def solution(mesh):
    in_specs = (
        P("win", None, "tile", None),
        P("win", None, "tile", None),
        P(None, "win", None, "tile", None),
        P("win", "tile"),
        P("win", "tile", None),
        P("win", "tile", None),
    )
    out_specs = (P("win", None, "tile", None), P("win", None, "tile", None))
    return jax.shard_map(
        functools.partial(on_device, mesh.shape["win"], mesh.shape["tile"]),
        mesh=mesh, in_specs=in_specs, out_specs=out_specs, check_vma=False
    )
```

```python
import functools

import jax
import jax.numpy as jnp
from jax import lax
from jax.experimental import pallas as pl
from jax.experimental.pallas import tpu as pltpu
from jax.sharding import PartitionSpec as P

ITERS = 3
EDGE = 8
MOMENTS = 2 * ITERS - 1

HOP, TILE_HOPS, BLOCK, SWAP_START, SWAP_FIELD, REDUCE, BEGIN = 2.40, (3.30, 1.50), 0.70, 2.20, 2.83, 5.31, 7.50


def doubling(length):
    steps, known = [], 1
    while known < length - 1:
        steps.append(known)
        known *= 2
    return steps


HINTS = {('back', 2): -1.4, 'early out': 1.3, ('model', 1): -0.87}
STEP = 1.00


class Steps:
    def __init__(self):
        self.todo = {}

    def add(self, name, needs, cost, run, sends=None, gets=None):
        self.todo[name] = (list(needs), cost, run, sends, gets)

    def order(self):
        senders = {sends[0]: name for name, (_, _, _, sends, _) in self.todo.items() if sends}
        after = {name: [] for name in self.todo}
        for name, (needs, _, _, _, gets) in self.todo.items():
            for need in needs:
                after[need].append((name, 0.0))
            if gets in senders:
                after[senders[gets]].append((name, self.todo[senders[gets]][3][2]))
        rank = {}

        def path(name):
            if name not in rank:
                rank[name] = self.todo[name][1] + max(
                    (wait + path(then) for then, wait in after[name]), default=0.0)
            return rank[name]

        for name in self.todo:
            path(name)
        for name in self.todo:
            kind = name if isinstance(name, str) else name[:2]
            rank[name] += HINTS.get(kind, 0.0)
        now, done, arrive, free, result = BEGIN, set(), {}, {}, []
        for _, (_, _, _, _, gets) in self.todo.items():
            if isinstance(gets, tuple) and gets[0] == "at":
                arrive[gets] = gets[1]
        left = dict(self.todo)
        while left:
            ready, soon = None, None
            for name, (needs, _, _, _, gets) in left.items():
                if any(need not in done for need in needs):
                    continue
                at = arrive.get(gets, None) if gets is not None else 0.0
                if at is None:
                    continue
                if at <= now:
                    if ready is None or rank[name] > rank[ready]:
                        ready = name
                elif soon is None or at < soon[0]:
                    soon = (at, name)
            pick = ready
            if pick is None:
                now, pick = soon
            _, cost, run, sends, _ = left.pop(pick)
            now += STEP * cost
            done.add(pick)
            if sends:
                message, link, latency, busy = sends
                begin = max(now, free.get(link, 0.0))
                free[link] = begin + busy
                arrive[message] = begin + busy + latency
            result.append((pick, run, now))
        return result


def two_sum(a, b):
    total = a + b
    back = total - a
    return total, (a - (total - back)) + (b - back)


def halves(a):
    big = 4097.0 * a
    high = big - (big - a)
    return high, a - high


def two_product(a, b):
    (ah, al), (bh, bl) = halves(a), halves(b)
    product = a * b
    return product, ((ah * bh - product) + ah * bl + al * bh) + al * bl


def pair_add(a, b):
    total, rest = two_sum(a[0], b[0])
    rest = rest + (a[1] + b[1])
    high = total + rest
    return high, rest - (high - total)


def pair_scale(a, factor):
    product, rest = two_product(a[0], factor)
    rest = rest + a[1] * factor
    high = product + rest
    return high, rest - (high - product)


def pair_rows(a, lo, hi):
    return a[0][lo:hi], a[1][lo:hi]


def pair_total(a):
    return jnp.sum(a[0], axis=1, keepdims=True) + jnp.sum(a[1], axis=1, keepdims=True)


def kernel(wins, tiles, rhs, err, cof, oblk_in, opos_in, owgt_in, x_out, r_out,
           obk, ops, owt, v, y, w, wn, c, d, ob, u, ui, vn, qb, qn, eo, ei, go, gi, rt, home, far, ahead,
           step, grad, energy, early, late, reds, lasts,
           x_sem, xs_sem, l_sem, f_recv, h_send, h_recv, b_send, b_recv, c_recv, g_send, g_recv,
           rt_send, rt_recv, rd_send, rd_recv, wn_send, wn_recv, hello):
    me_w = lax.axis_index("win")
    me_t = lax.axis_index("tile")
    lev = lax.rem(me_w, 2)
    other = 1 - lev
    mate = me_w + 1 - 2 * lev
    has_next = me_w + 2 < wins
    has_prev = me_w >= 2
    rows, cols = v.shape[1], v.shape[2]
    count = wins * tiles
    me = me_w * tiles + me_t
    width = ops.shape[2]
    nblk = ops.shape[1]
    last = rows - 1
    blocks = rows // EDGE
    final = blocks - 1
    pieces = list(range(final - 1)) + [final, final - 1]
    many = len(pieces)
    f32 = jnp.float32

    odd = lax.rem(me_t, 2)
    even = odd == 0

    def first_row(k):
        return pl.multiple_of((k + odd * (final - 2 * k)) * EDGE, EDGE)

    def rowset(k):
        return pl.ds(first_row(k), EDGE)

    def row_beyond(k, side):
        return pl.ds(first_row(k) - 1 + 9 * odd if side == 0 else first_row(k) + EDGE - 9 * odd, 1)

    def edge_row(side):
        return pl.ds(odd * last if side == 0 else last - odd * last, 1)

    beside = (me_t - 1 + 2 * odd, me_t + 1 - 2 * odd)
    ways = tuple(jnp.logical_and(tile >= 0, tile < tiles) for tile in beside)

    def remote(src, dst, ssem, rsem, win, tile):
        return pltpu.make_async_remote_copy(
            src_ref=src, dst_ref=dst, send_sem=ssem, recv_sem=rsem,
            device_id=(win, tile), device_id_type=pl.DeviceIdType.MESH)

    def all_of(ref, sem):
        return pltpu.make_async_copy(ref, ref, sem)

    barrier = pltpu.get_barrier_semaphore()

    def signal(sem, win, tile):
        pl.semaphore_signal(sem, inc=1, device_id=(win, tile), device_id_type=pl.DeviceIdType.MESH)

    def greet(sem, ends):
        for there, win, tile in ends:
            pl.when(there)(functools.partial(signal, sem, win, tile))

    def met(sem, ends):
        pl.semaphore_wait(sem, sum(there.astype(jnp.int32) for there, _, _ in ends))

    def along_tile(hop):
        return [(me_t >= hop, me_w, me_t - hop), (me_t + hop < tiles, me_w, me_t + hop)]

    def along_win(hop):
        return [(me_w >= 2 * hop, me_w - 2 * hop, me_t),
                (me_w + 2 * hop < wins, me_w + 2 * hop, me_t)]

    facing = [(me_w >= 0, mate, me_t)]
    near = facing + along_tile(1) + along_win(1)
    rounds = ([along_tile(hop) for hop in doubling(tiles)] + [facing]
              + [along_win(hop) for hop in doubling(wins // 2)])

    greet(barrier, near)

    swaps = [
        remote(rhs.at[0, other], v.at[lev], xs_sem.at[0], x_sem.at[0], mate, me_t),
        remote(err.at[0, other], w.at[lev], xs_sem.at[0], x_sem.at[1], mate, me_t),
    ] + [
        remote(cof.at[:, 0, other, rowset(k)], c.at[:, lev, rowset(k)],
               xs_sem.at[0], x_sem.at[3 + n], mate, me_t)
        for n, k in enumerate(pieces)
    ]
    arrivals = [
        remote(rhs.at[0, other], v.at[other], xs_sem.at[0], x_sem.at[0], mate, me_t),
        remote(err.at[0, other], w.at[other], xs_sem.at[0], x_sem.at[1], mate, me_t),
    ] + [
        remote(cof.at[:, 0, other, rowset(k)], c.at[:, other, rowset(k)],
               xs_sem.at[0], x_sem.at[3 + n], mate, me_t)
        for n, k in enumerate(pieces)
    ]
    locs = {
        "block": pltpu.make_async_copy(oblk_in, obk, l_sem.at[0]),
        "pos": pltpu.make_async_copy(opos_in, ops, l_sem.at[1]),
        "weight": pltpu.make_async_copy(owgt_in, owt, l_sem.at[4]),
        "rhs": pltpu.make_async_copy(rhs.at[0, lev], v.at[lev], l_sem.at[2]),
        "err": pltpu.make_async_copy(err.at[0, lev], w.at[lev], l_sem.at[3]),
        "home": pltpu.make_async_copy(rhs.at[0, other], home, l_sem.at[3]),
        "cof": pltpu.make_async_copy(cof.at[:, 0, lev], c.at[:, lev], l_sem.at[3]),
        "far": pltpu.make_async_copy(cof.at[:, 0, other, rowset(pieces[-1])], far, l_sem.at[5]),
    }
    for one in locs.values():
        one.start()
    met(barrier, near)
    for one in swaps[:3]:
        one.start()
    greet(hello.at[0], rounds[0])

    for side in range(2):
        @pl.when(jnp.logical_not(ways[side]))
        def _():
            for it in range(ITERS):
                ei[it, side] = jnp.zeros(ei.shape[2:], f32)
                gi[it, side] = jnp.zeros(gi.shape[2:], f32)

    @pl.when(jnp.logical_not(has_prev))
    def _():
        for it in range(ITERS):
            ui[it] = jnp.zeros(ui.shape[1:], f32)

    @pl.when(jnp.logical_not(has_next))
    def _():
        wn[...] = jnp.zeros(wn.shape, f32)
        for it in range(ITERS):
            vn[it] = jnp.zeros(vn.shape[1:], f32)

    states = (v, y.at[0], y.at[1])
    row8 = lax.broadcasted_iota(jnp.int32, (EDGE, cols), 0)

    def east(a):
        return pltpu.roll(a, cols - 1, 1)

    def west(a):
        return pltpu.roll(a, 1, 1)

    def sides(a, beyond):
        top, bottom = jnp.where(even, beyond[0], beyond[1]), jnp.where(even, beyond[1], beyond[0])
        return (jnp.where(row8 == 0, top, pltpu.roll(a, 1, 0))
                + jnp.where(row8 == EDGE - 1, bottom, pltpu.roll(a, EDGE - 1, 0)))

    def edge_copy(out, into, ssem, rsem, it, side, i):
        return remote(out.at[it, side, i], into.at[it, side, i], ssem.at[side],
                      rsem(it, side, i), me_w, beside[side])

    def edge_sem(it, side, i):
        return f_recv.at[side] if it == 0 else h_recv.at[it - 1, side, i]

    def adjoint_sem(it, side, i):
        return g_recv.at[it, side, i]


    def back_copy(it, k):
        return remote(states[it].at[0, rowset(k)], vn.at[it, rowset(k)],
                      b_send.at[0], b_recv.at[it - 1, k] if it else f_recv.at[2], me_w - 2, me_t)

    def forth_copy(it, k):
        return remote(u.at[it, 1, rowset(k)], ui.at[it, rowset(k)],
                      b_send.at[2 if it else 1], c_recv.at[it, k], me_w + 2, me_t)

    def ret_copy(it, k):
        return remote(y.at[it, other, rowset(k)], rt.at[it, rowset(k)],
                      rt_send, rt_recv.at[k if it == ITERS - 1 else blocks], mate, me_t)

    sends_ahead = jnp.logical_and(lev == 1, has_next)

    def ahead_copy(n):
        return remote(ahead.at[n], ui.at[0, rowset(pieces[-1])], b_send.at[3],
                      c_recv.at[0, pieces[-1]], me_w + 2 - n, me_t)

    wn_copy = remote(w.at[0], wn, wn_send, wn_recv, me_w - 2, me_t)

    def end_side(k):
        return 0 if k == 0 else 1 if k == final else None

    def model(it, i, k):
        src, at = states[it], rowset(k)
        a = src[i, at]
        beyond = [ei[it, side, i] if side == end_side(k) else src[i, row_beyond(k, side)]
                  for side in range(2)]
        u[it, i, at] = (c[0, i, at] * a + c[1, i, at] * sides(a, beyond)
                        + c[2, i, at] * east(a) + c[3, i, at] * west(a))
        if i == 1 and (it, k) != (0, pieces[-1]):
            pl.when(has_next)(forth_copy(it, k).start)

    def misfit_here(it, k):
        at = rowset(k)
        qb[it, at] = w[1, at] * (states[it][1, at] - u[it, 0, at])

    def misfit_next(it, k):
        at = rowset(k)
        qn[it, at] = wn[at] * (vn[it, at] - u[it, 1, at])

    def adjoint(it, i, q, k, alone=None):
        at = rowset(k)
        a = q[it, at]
        beyond = []
        for side in range(2):
            if side == end_side(k):
                beyond.append(gi[it, side, i])
            elif alone is not None:
                beyond.append(jnp.zeros((1, cols), f32))
            else:
                row = row_beyond(k, side)
                beyond.append(c[1, i, row] * q[it, row])
        return (c[0, i, at] * a + sides(c[1, i, at] * a, beyond)
                + west(c[2, i, at] * a) + east(c[3, i, at] * a))

    def image(it, i, k, alone=None):
        at = rowset(k)
        src = states[it]
        if i == 1:
            return (qb[it, at] + d[1, at] * src[1, at]) - adjoint(it, 1, qn, k, alone)
        return (d[0, at] * src[0, at] - adjoint(it, 0, qb, k, alone)) + w[0, at] * (src[0, at] - ui[it, at])

    def diagonal():
        ob_back.wait_recv()
        per_row = cols // width
        base = lev * (rows * per_row)
        spot = lax.broadcasted_iota(jnp.int32, (rows, nblk), 0) * per_row + base
        for i in range(2):
            who = ob[i, nblk:nblk + 1, 0:nblk]
            sums = ob[i, 0:nblk, :]
            for k in range(per_row):
                hot = jnp.where((spot + k).astype(f32) == who, 1.0, 0.0)
                d[i, :, k * width:(k + 1) * width] = jnp.dot(
                    hot, sums, precision=lax.Precision.HIGHEST, preferred_element_type=f32)

    def lanes(a, b):
        total = None
        for k in range(blocks):
            at = slice(k * EDGE, (k + 1) * EDGE)
            here = a[0, at] * b[0, at] + a[1, at] * b[1, at]
            total = here if total is None else total + here
        return folded(total)

    def folded(total):
        total = jnp.sum(total, axis=0, keepdims=True)
        parts = [total[:, k * width:(k + 1) * width] for k in range(cols // width)]
        while len(parts) > 1:
            parts = [sum(parts[k:k + 2]) for k in range(0, len(parts), 2)]
        return parts[0]

    def to_all(part, into, sems):
        turned = 2 * me < count

        def send(o, carry):
            to = lax.rem(me + jnp.where(turned, count - o, o), count)
            remote(part, into.at[me], rd_send.at[sems], rd_recv.at[sems],
                   to // tiles, lax.rem(to, tiles)).start()
            return carry

        lax.fori_loop(1, count, send, 0)
        into[me] = part[...]

    def from_all(into, sems):
        most = into.at[pl.ds(0, count - 1)]
        pltpu.make_async_copy(most, most, rd_recv.at[sems]).wait()
        high, low = into[0], jnp.zeros(into.shape[1:], f32)
        for k in range(1, count):
            high, rest = two_sum(high, into[k])
            low = low + rest
        return high, low

    def edges_out(it, side, i):
        if it == 0:
            eo[it, side, i] = v[i, edge_row(side)]
        else:
            whole = image(it - 1, i, 0 if side == 0 else final, alone=True)
            low, high = whole[0:1], whole[EDGE - 1:EDGE]
            eo[it, side, i] = jnp.where(even, low, high) if side == 0 else jnp.where(even, high, low)
        pl.when(ways[side])(edge_copy(eo, ei, h_send, edge_sem, it, side, i).start)

    for one in ("block", "pos", "weight"):
        locs[one].wait()
    cell = lax.broadcasted_iota(jnp.int32, (width, width), 0)
    ones = jnp.ones((8, width), f32)
    ob[lev, nblk:, :] = jnp.zeros((8, width), f32)

    def per_block(b, carry):
        hit = jnp.where(cell == ops[0, pl.ds(b, 1), :], owt[0, pl.ds(b, 1), :], 0.0)
        total = lax.dot_general(ones, hit, (((1,), (1,)), ((), ())),
                                precision=lax.Precision.HIGHEST,
                                preferred_element_type=f32)
        ob[lev, pl.ds(b, 1), :] = total[0:1]
        return carry

    most = nblk // 2
    lax.fori_loop(0, most, per_block, 0)
    locs["rhs"].wait()
    arrivals[0].wait_recv()
    swaps[3].start()
    for k in range(blocks):
        pl.when(has_prev)(back_copy(0, k).start)
    for side in range(2):
        for i in range(2):
            edges_out(0, side, i)
    all_of(y, l_sem.at[3]).wait()
    locs["far"].wait()

    @pl.when(sends_ahead)
    def _():
        at = rowset(pieces[-1])
        rims = [row_beyond(pieces[-1], side) for side in range(2)]
        for n, (a, beyond, k) in enumerate((
                (v[lev, at], [v[lev, row] for row in rims], [c[m, lev, at] for m in range(4)]),
                (home[at], [home[row] for row in rims], [far[m] for m in range(4)]))):
            ahead[n] = k[0] * a + k[1] * sides(a, beyond) + k[2] * east(a) + k[3] * west(a)
            ahead_copy(n).start()

    lax.fori_loop(most, nblk, per_block, 0)
    ob[lev, nblk:nblk + 1, 0:nblk] = obk[...].astype(f32)
    ob_copy = remote(ob.at[lev], ob.at[lev], xs_sem.at[1], x_sem.at[2], mate, me_t)
    ob_back = remote(ob.at[lev], ob.at[other], xs_sem.at[1], x_sem.at[2], mate, me_t)
    ob_copy.start()
    for one in swaps[4:]:
        one.start()

    S = Steps()
    scalars = {}

    def spread(at):
        met(hello.at[at], rounds[at])
        if at + 1 < len(rounds):
            greet(hello.at[at + 1], rounds[at + 1])

    for n in range(len(rounds)):
        S.add(("spread", n), [("spread", n - 1)] if n else [], 0.05, functools.partial(spread, n),
              sends=(("hello", n), "hello", 3.0, 0.0), gets=("hello", n - 1) if n else ("at", 1.5))
    met_all = [("spread", len(rounds) - 1)]

    S.add("here", [], 0.0, lambda: None)

    def err_there():
        arrivals[1].wait_recv()
        pl.when(has_prev)(wn_copy.start)

    S.add("err there", ["here"], 0.03, err_there, sends=("next weights", "weights", 4.8, 0.0),
          gets=("at", SWAP_START + 2 * SWAP_FIELD))
    S.add("next weights", [], 0.01, lambda: pl.when(has_next)(wn_copy.wait_recv), gets="next weights")
    S.add("diagonal", [], 0.6, diagonal, gets=("at", 15.2))

    for n, k in enumerate(pieces):
        S.add(("cof", k), ["here"], 0.02, arrivals[2 + n].wait_recv,
              gets=("at", SWAP_START + SWAP_FIELD * (2 + 4.0 * (n + 1) / many)))

    def whole_rows(it, i, k):
        if it == 0:
            return []
        return [("image", it - 1, i, k)]

    def adjoint_out(it, side, i):
        row = edge_row(side)
        go[it, side, i] = c[1, i, row] * (qn if i else qb)[it, row]
        pl.when(ways[side])(edge_copy(go, gi, g_send, adjoint_sem, it, side, i).start)

    def edges_in(out, into, ssem, rsem, it, side, i):
        pl.when(ways[side])(edge_copy(out, into, ssem, rsem, it, side, i).wait_recv)

    def store_image(it, i, k):
        y[it, i, rowset(k)] = image(it, i, k)
        if i == 0 and it + 1 < ITERS:
            pl.when(has_prev)(back_copy(it + 1, k).start)

    for it in range(ITERS):
        for side, k in ((0, 0), (1, final)):
            for i in range(2):
                if it > 0:
                    needs = [("here", it - 1, k), ("adjoint in", it - 1, side, i), "diagonal"]
                    needs += [("next", it - 1, k)] if i else [("forth", it - 1, k)]
                    S.add(("edges out", it, side, i), needs, 0.06, functools.partial(edges_out, it, side, i),
                          sends=(("edges", it, side, i), ("tile", side), TILE_HOPS[side], 0.05))
                if it > 0:
                    S.add(("edges in", it, side, i), [], 0.02,
                          functools.partial(edges_in, eo, ei, h_send, edge_sem, it, side, i),
                          gets=("edges", it, side, i))
                elif i == 0:
                    S.add(("edges in", 0, side), [], 0.02, functools.partial(
                        pl.when(ways[side]), all_of(ei.at[0, side], f_recv.at[side]).wait), gets=("at", 7.7))
                S.add(("adjoint out", it, side, i), [("next" if i else "here", it, k)], 0.03,
                      functools.partial(adjoint_out, it, side, i),
                      sends=(("adjoint", it, side, i), ("tile", side), TILE_HOPS[side], 0.05))
                S.add(("adjoint in", it, side, i), [], 0.02,
                      functools.partial(edges_in, go, gi, g_send, adjoint_sem, it, side, i),
                      gets=("adjoint", it, side, i))
        for k in range(blocks):
            if it > 0:
                S.add(("back", it, k), [], 0.02, lambda it=it, k=k: pl.when(has_next)(
                    back_copy(it, k).wait_recv), gets=("back", it, k))
            elif k == 0:
                S.add(("back", 0), [], 0.02, functools.partial(
                    pl.when(has_next), all_of(vn.at[0], f_recv.at[2]).wait), gets=("at", 10.2))
            S.add(("forth", it, k), [], 0.02, lambda it=it, k=k: pl.when(has_prev)(
                forth_copy(it, k).wait_recv),
                  gets=("at", 10.5) if (it, k) == (0, pieces[-1]) else ("forth", it, k))
            around = [m for m in (k - 1, k, k + 1) if 0 <= m < blocks]
            ends = [side for side, m in ((0, 0), (1, final)) if m == k]
            for i in range(2):
                needs = [("cof", k)] + [("edges in", it, side) + ((i,) if it else ()) for side in ends]
                for m in around:
                    needs += whole_rows(it, i, m)
                S.add(("model", it, i, k), needs, 0.05, functools.partial(model, it, i, k),
                      sends=(("forth", it, k), "forth", HOP, BLOCK)
                      if i == 1 and (it, k) != (0, pieces[-1]) else None)
                needs = ["diagonal", "here", "err there"] + [("adjoint in", it, side, i) for side in ends]
                needs += [("next" if i else "here", it, m) for m in around]
                needs += [("here", it, k)] if i else [("forth", it, k)]
                S.add(("image", it, i, k), needs, 0.06, functools.partial(store_image, it, i, k),
                      sends=(("back", it + 1, k), "back", HOP, BLOCK) if i == 0 and it + 1 < ITERS else None)
            S.add(("here", it, k), ["here", "err there", ("model", it, 0, k)] + whole_rows(it, 1, k), 0.03,
                  functools.partial(misfit_here, it, k))
            S.add(("next", it, k), ["next weights", ("model", it, 1, k), ("back", it) + ((k,) if it else ())], 0.03,
                  functools.partial(misfit_next, it, k))
            S.add(("ret out", it, k), [("image", it, 0, k), ("image", it, 1, k)], 0.02,
                  lambda it=it, k=k: ret_copy(it, k).start(),
                  sends=(("ret", it, k), "ret", HOP, BLOCK))
            if it == ITERS - 1:
                S.add(("ret", it, k), [], 0.01, ret_copy(it, k).wait_recv, gets=("ret", it, k))

    S.add("ret", ["early in"], 0.01, all_of(rt.at[pl.ds(0, ITERS - 1)], rt_recv.at[blocks]).wait)

    def images(it):
        return [("image", it, i, k) for i in range(2) for k in range(blocks)]

    def moment(n, a, b):
        early[n:n + 1] = lanes(a, b)

    S.add("moment 0", [], 0.15, lambda: moment(0, v, v))
    S.add("moment 1", images(0), 0.3, lambda: (moment(1, v, y.at[0]), moment(2, y.at[0], y.at[0])))
    S.add("moment 3", images(1), 0.3,
          lambda: (moment(3, y.at[0], y.at[1]), moment(4, y.at[1], y.at[1])))

    S.add("early out", ["moment 0", "moment 1", "moment 3", *[("model", 2, 1, k) for k in range(blocks)]] + met_all, 0.4,
          lambda: to_all(early, reds, 0), sends=("early", "all", REDUCE, 0.0))

    def energy_states():
        total = None
        first = jnp.where(has_prev, 0.0, 1.0)
        for k in range(blocks):
            at = slice(k * EDGE, (k + 1) * EDGE)
            a, b = states[2][0, at], states[2][1, at]
            here = (d[0, at] + first * w[0, at]) * (a * a) + d[1, at] * (b * b)
            total = here if total is None else total + here
        energy[...] = total

    def energy_misfits(k):
        at = rowset(k)
        energy[...] += (qb[2, at] * (states[2][1, at] - u[2, 0, at])
                        + qn[2, at] * (vn[2, at] - u[2, 1, at]))

    def late_out():
        late[...] = folded(energy[...])
        to_all(late, lasts, 1)

    S.add("energy", images(1), 0.1, energy_states)
    for k in range(blocks):
        S.add(("energy", k), ["energy", ("here", 2, k), ("next", 2, k)], 0.04,
              functools.partial(energy_misfits, k))
    S.add("late out", [("energy", k) for k in range(blocks)] + met_all, 0.5, late_out,
          sends=("late", "all", REDUCE, 0.0))

    def early_in():
        m = from_all(reds, 0)
        plain = jnp.sum(m[0], axis=1, keepdims=True)
        g0 = plain[0:1]
        a0 = g0 / plain[1:2]
        less = pair_add(pair_rows(m, 0, 4), pair_scale(pair_rows(m, 1, 5), -a0))
        less = pair_add(pair_rows(less, 0, 3), pair_scale(pair_rows(less, 1, 4), -a0))
        one = pair_total(less)
        g1, d1 = one[0:1], one[1:2]
        b1 = g1 / g0
        a1 = g1 / (d1 - b1 * g1 / a0)
        p1 = -(a0 + a1 + a1 * b1)
        p2 = a0 * a1
        q = pair_add(pair_add(pair_rows(m, 0, 3), pair_scale(pair_rows(m, 1, 4), p1)),
                     pair_scale(pair_rows(m, 2, 5), p2))
        g2 = pair_total(pair_add(pair_add(pair_rows(q, 0, 1), pair_scale(pair_rows(q, 1, 2), p1)),
                                 pair_scale(pair_rows(q, 2, 3), p2)))
        rest = pair_add(pair_rows(m, 3, 4), pair_scale(pair_rows(m, 4, 5), p1))
        base = pair_add(pair_add(pair_rows(q, 1, 2), pair_scale(pair_rows(q, 2, 3), p1)),
                        pair_scale(rest, p2))
        scalars.update(a0=a0, a1=a1, b1=b1, p1=p1, p2=p2, g2=g2, b2=g2 / g1, base=base)

    S.add("early in", ["late out"], 0.6, early_in, gets="early")

    def late_in():
        s = scalars
        m = from_all(lasts, 1)
        d2 = pair_total(pair_add(s["base"], pair_scale(pair_scale(m, s["p2"]), s["p2"])))
        scalars["a2"] = s["g2"] / (d2 - s["b2"] * s["g2"] / s["a1"])

    S.add("late in", ["early in", "sent"], 0.4, late_in, gets="late")

    def own(level):
        return lambda at: v[level, at], lambda it, at: y[it, level, at]

    def away():
        return lambda at: home[at], lambda it, at: rt[it, at]

    def solve(level, source, k):
        s = scalars
        at = rowset(k)
        first, images_of = source
        r0, y0, y1 = first(at), images_of(0, at), images_of(1, at)
        p = (r0 - s["a0"] * y0) + s["b1"] * r0
        r2 = (r0 + s["p1"] * y0) + s["p2"] * y1
        x_out[0, level, at] = s["a0"] * r0 + s["a1"] * p
        r_out[0, level, at] = r2
        step[level, at] = r2 + s["b2"] * p

    def tail(level, source, k):
        s = scalars
        at = rowset(k)
        _, images_of = source
        y0, y1, y2 = images_of(0, at), images_of(1, at), images_of(2, at)
        s1 = (y0 - s["a0"] * y1) + s["b1"] * y0
        grad[level, at] = ((y0 + s["p1"] * y1) + s["p2"] * y2) + s["b2"] * s1

    def finish(level, k):
        at = rowset(k)
        x_out[0, level, at] = x_out[0, level, at] + scalars["a2"] * step[level, at]
        r_out[0, level, at] = r_out[0, level, at] - scalars["a2"] * grad[level, at]

    for k in range(blocks):
        S.add(("solve own", k), ["early in"] + [("image", it, i, k) for it in range(2) for i in range(2)],
              0.06, functools.partial(solve, lev, own(lev), k))
        S.add(("solve away", k), ["early in", "here", "ret"],
              0.06, functools.partial(solve, other, away(), k))
        S.add(("tail own", k), ["early in"] + [("image", it, i, k) for it in range(3) for i in range(2)],
              0.06, functools.partial(tail, lev, own(lev), k))
        S.add(("tail away", k), ["early in", "ret", ("ret", ITERS - 1, k)],
              0.06, functools.partial(tail, other, away(), k))
        S.add(("finish own", k), ["late in", ("solve own", k), ("tail own", k)],
              0.04, functools.partial(finish, lev, k))
        S.add(("finish away", k), ["late in", ("solve away", k), ("tail away", k)],
              0.04, functools.partial(finish, other, k))

    def sent():
        all_of(y, xs_sem.at[0]).wait()
        ob_copy.wait_send()
        pl.when(has_prev)(wn_copy.wait_send)
        for side in range(2):
            pl.when(ways[side])(all_of(eo.at[:, side], h_send.at[side]).wait)
            pl.when(ways[side])(all_of(go.at[:, side], g_send.at[side]).wait)
        all_of(rt, rt_send).wait()
        pl.when(has_prev)(all_of(vn, b_send.at[0]).wait)
        pl.when(has_next)(all_of(ui.at[0, pl.ds(0, rows - EDGE)], b_send.at[1]).wait)
        pl.when(has_next)(all_of(ui.at[pl.ds(1, ITERS - 1)], b_send.at[2]).wait)
        pl.when(sends_ahead)(all_of(ahead, b_send.at[3]).wait)
        all_of(reds.at[pl.ds(0, count - 1)], rd_send.at[0]).wait()

    S.add("sent", [("tail away", k) for k in range(blocks)], 0.5, sent)
    order = S.order()
    for name, run, _ in order:
        run()

    most = lasts.at[pl.ds(0, count - 1)]
    pltpu.make_async_copy(most, most, rd_send.at[1]).wait()


def on_device(wins, tiles, right_side, error_weight, coeffs, obs_block, obs_pos, obs_weight):
    _, levels, rows, cols = right_side.shape
    nblk, width = obs_pos.shape[1:]
    f32 = jnp.float32
    vm = functools.partial(pltpu.VMEM, dtype=f32)
    dma = pltpu.SemaphoreType.DMA
    hbm = pl.BlockSpec(memory_space=pltpu.HBM)
    vmem = pl.BlockSpec(memory_space=pltpu.VMEM)
    blocks = rows // EDGE
    field = (rows, cols)
    edge = vm((ITERS, 2, 2, 1, cols))
    scratch = [
        pltpu.VMEM(obs_block.shape, jnp.int32),
        pltpu.VMEM(obs_pos.shape, jnp.int32),
        vm(obs_weight.shape),
        vm((2,) + field),
        vm((ITERS, 2) + field),
        vm((2,) + field),
        vm(field),
        vm((4, 2) + field),
        vm((2,) + field),
        vm((2, nblk + 8, width)),
        vm((ITERS, 2) + field),
        vm((ITERS,) + field),
        vm((ITERS,) + field),
        vm((ITERS,) + field),
        vm((ITERS,) + field),
        edge, edge, edge, edge,
        vm((ITERS,) + field),
        vm(field),
        vm((4, EDGE, cols)),
        vm((2, EDGE, cols)),
        vm((2,) + field),
        vm((2,) + field),
        vm((EDGE, cols)),
        vm((MOMENTS, width)),
        vm((1, width)),
        vm((wins * tiles, MOMENTS, width)),
        vm((wins * tiles, 1, width)),
        dma((3 + blocks,)), dma((2,)), dma((6,)),
        dma((3,)), dma((2,)), dma((ITERS - 1, 2, 2)),
        dma((4,)), dma((ITERS - 1, blocks)), dma((ITERS, blocks)),
        dma((2,)), dma((ITERS, 2, 2)),
        dma, dma((1 + blocks,)),
        dma((2,)), dma((2,)),
        dma, dma,
        pltpu.SemaphoreType.REGULAR((1 + len(doubling(tiles)) + len(doubling(wins // 2)),)),
    ]
    out = vm(right_side.shape)
    return pl.pallas_call(
        functools.partial(kernel, wins, tiles),
        out_shape=(out, out),
        in_specs=[hbm] * 6,
        out_specs=(vmem, vmem),
        scratch_shapes=scratch,
        compiler_params=pltpu.CompilerParams(has_side_effects=True, collective_id=0,
                                             vmem_limit_bytes=60 * 1024 * 1024),
    )(right_side, error_weight, coeffs, obs_block, obs_pos, obs_weight)


def solution(mesh):
    in_specs = (
        P("win", None, "tile", None),
        P("win", None, "tile", None),
        P(None, "win", None, "tile", None),
        P("win", "tile"),
        P("win", "tile", None),
        P("win", "tile", None),
    )
    out_specs = (P("win", None, "tile", None), P("win", None, "tile", None))
    return jax.shard_map(
        functools.partial(on_device, mesh.shape["win"], mesh.shape["tile"]),
        mesh=mesh, in_specs=in_specs, out_specs=out_specs, check_vma=False
    )
```
